32 devices in a mesh: dp: 8 (over z, x), mp: 4 (over y, core).
Axes of the slice: x: 2, y: 2, z: 4, core: 2. Of those that a mesh axis runs over, the one named last changes fastest.
Arguments:
- hidden_in: bfloat16 [8192, 1024], P(('dp', 'mp')), may hold values from -6 to 6
- seg_lengths: int32 [8, 8], P('dp'), may hold values from 1 to 256, 1024 in all within a row
- partner: int32 [8, 8], P('dp'), may hold values from 0 to 7, as said below
- qkv_weight: float32 [2, 1024, 3, 1024], P(None, 'dp', None, 'mp'), may hold values from -0.1875 to 0.1875
- out_weight: float32 [2, 1024, 1024], P(None, 'mp', 'dp'), may hold values from -2 to 2
- up_weight: float32 [2, 1024, 4096], P(None, 'dp', 'mp'), may hold values from -0.1875 to 0.1875
- down_weight: float32 [2, 4096, 1024], P(None, 'mp', 'dp'), may hold values from -0.09375 to 0.09375
- norm_params: float32 [2, 2, 2, 1024], P(None, None, None, 'dp'), may hold values from -0.6 to 1.15, as said below
- emb_weight: float32 [1024, 128], P('dp'), may hold values from -0.1875 to 0.1875
- log_scale: float32 [1], replicated, may hold values from 2.5 to 3.2
- qkv_moments: float32 [2, 2, 1024, 3, 1024], P(None, None, 'dp', None, 'mp'), as said below
- out_moments: float32 [2, 2, 1024, 1024], P(None, None, 'mp', 'dp'), as said below
- up_moments: float32 [2, 2, 1024, 4096], P(None, None, 'dp', 'mp'), as said below
- down_moments: float32 [2, 2, 4096, 1024], P(None, None, 'mp', 'dp'), as said below
- norm_moments: float32 [2, 2, 2, 2, 1024], P(None, None, None, None, 'dp'), as said below
- emb_moments: float32 [2, 1024, 128], P(None, 'dp'), as said below
- scale_moments: float32 [2, 1], replicated, as said below
Outputs:
- hidden_out: float32 [8192, 1024], P(('dp', 'mp'))
- hidden_grad: float32 [8192, 1024], P(('dp', 'mp'))
- loss: float32 [1], replicated
- clip_norm: float32 [1], replicated
- qkv_new: float32 [2, 1024, 3, 1024], P(None, 'dp', None, 'mp')
- qkv_first: float32 [2, 1024, 3, 1024], P(None, 'dp', None, 'mp')
- qkv_second: float32 [2, 1024, 3, 1024], P(None, 'dp', None, 'mp')
- out_new: float32 [2, 1024, 1024], P(None, 'mp', 'dp')
- out_first: float32 [2, 1024, 1024], P(None, 'mp', 'dp')
- out_second: float32 [2, 1024, 1024], P(None, 'mp', 'dp')
- up_new: float32 [2, 1024, 4096], P(None, 'dp', 'mp')
- up_first: float32 [2, 1024, 4096], P(None, 'dp', 'mp')
- up_second: float32 [2, 1024, 4096], P(None, 'dp', 'mp')
- down_new: float32 [2, 4096, 1024], P(None, 'mp', 'dp')
- down_first: float32 [2, 4096, 1024], P(None, 'mp', 'dp')
- down_second: float32 [2, 4096, 1024], P(None, 'mp', 'dp')
- norm_new: float32 [2, 2, 2, 1024], P(None, None, None, 'dp')
- norm_first: float32 [2, 2, 2, 1024], P(None, None, None, 'dp')
- norm_second: float32 [2, 2, 2, 1024], P(None, None, None, 'dp')
- emb_new: float32 [1024, 128], P('dp')
- emb_first: float32 [1024, 128], P('dp')
- emb_second: float32 [1024, 128], P('dp')
- scale_new: float32 [1], replicated
- scale_first: float32 [1], replicated
- scale_second: float32 [1], replicated
The draws below stay inside these ranges and needn't reach their ends.
Inputs may be any that keep to these rules, and one draw needn't show every extreme that they name: `seg_lengths`: the 8 lengths of a row sum to 1024. The segments of a row come in pairs: partner of s is never s, and the partner of the partner of s is s. `norm_params`: gains near 1 at index 0 of the third dimension, biases of both signs at index 1. `qkv_moments`: index 0 holds first moments of both signs, index 1 positive second moments. `out_moments`: index 0 holds first moments of both signs, index 1 positive second moments. `up_moments`: index 0 holds first moments of both signs, index 1 positive second moments. `down_moments`: index 0 holds first moments of both signs, index 1 positive second moments. `norm_moments`: index 0 holds first moments of both signs, index 1 positive second moments. `emb_moments`: index 0 holds first moments of both signs, index 1 positive second moments. `scale_moments`: index 0 holds the first moment, index 1 the positive second moment.
All inputs are finite; a program needn't handle non-finite values.
Results may differ from the reference program's by a relative error of at most 0.018.
Values may be sent and summed in bfloat16 or wider, within the bound.
No kernel may reach another device: no remote copies, remote signals or barrier semaphores. Data moves between devices by JAX's collectives and lax.ppermute only.
A program may use at most 192 MiB of HBM per device.

```python
import math
import jax
import jax.numpy as jnp
import numpy as np
from jax import lax

D = 1024
HEAD_DIM = 64
FF = 4096
EMB = 128
LAYERS = 2
STEP = 5
ROW_LEN = 1024
SEGS = 8
ROWS = 8
TOKENS = 8192


def gradient_size():
    params_all = LAYERS * (4 * D * D + 2 * D * FF + 4 * D) + D * EMB + 1
    return params_all ** (-0.5)


def moment_pair(key, shape, typical):
    key_one, key_two = jax.random.split(key)
    moment_one = 0.11 * typical * jax.random.truncated_normal(key_one, -3.0, 3.0, shape, jnp.float32)
    spread = jax.random.uniform(key_two, shape, jnp.float32, 0.0, 1.3862944)
    moment_two = 0.053 * typical * typical * jnp.exp(spread)
    return jnp.stack([moment_one, moment_two])


def draw_partner(key, part):

    def pair_row(row_key):
        order = jax.random.permutation(row_key, SEGS).astype(jnp.int32)
        swapped = order.reshape(SEGS // 2, 2)[:, ::-1].reshape(SEGS)
        return jnp.zeros((SEGS,), jnp.int32).at[order].set(swapped)
    return jax.vmap(pair_row)(jax.random.split(key, ROWS))


def draw_norm_params(key, part):
    key_one, key_two = jax.random.split(key)
    gains = 1.0 + jax.random.uniform(key_one, (LAYERS, 2, 1, D), jnp.float32, -0.15, 0.15)
    biases = 0.2 * jax.random.truncated_normal(key_two, -3.0, 3.0, (LAYERS, 2, 1, D), jnp.float32)
    return jnp.concatenate([gains, biases], axis=2)


def draw_qkv_moments(key, part):
    return moment_pair(key, (LAYERS, D, 3, D), gradient_size())


def draw_out_moments(key, part):
    return moment_pair(key, (LAYERS, D, D), gradient_size())


def draw_up_moments(key, part):
    return moment_pair(key, (LAYERS, D, FF), gradient_size())


def draw_down_moments(key, part):
    return moment_pair(key, (LAYERS, FF, D), gradient_size())


def draw_norm_moments(key, part):
    return moment_pair(key, (LAYERS, 2, 2, D), gradient_size())


def draw_emb_moments(key, part):
    return moment_pair(key, (D, EMB), 3.0 * gradient_size())


def draw_scale_moments(key, part):
    return moment_pair(key, (1,), 30.0 * gradient_size())


def block_levels(own_key, shape, shards, smallest, largest):
    loudness = 1.0
    for axis_at, blocks in shards:
        heights = jax.random.uniform(jax.random.fold_in(jax.random.fold_in(own_key, 6), axis_at), (blocks,), jnp.float32, smallest / len(shards), largest / len(shards))
        loudness = loudness * jnp.repeat(jnp.exp(heights), shape[axis_at] // blocks).reshape((-1,) + (1,) * (len(shape) - 1 - axis_at))
    return loudness


def length_profile(count, total, reach, slope):
    portions = [(1 << 20) // math.isqrt(rank ** slope) + 1 for rank in range(2, count + 1)]
    spare, given = total - reach - (count - 1), [1] * (count - 1)
    while spare > 0:
        candidates = [i for i in range(count - 1) if given[i] < reach]
        whole, budget = sum([portions[i] for i in candidates]), spare
        for i in candidates:
            addition = min(reach - given[i], max(1, budget * portions[i] // whole), spare)
            given[i] = given[i] + addition
            spare = spare - addition
    return np.array([reach] + given)


def uneven_parts(stream_key, count, total, bound, skew):
    if count == 2:
        one = jax.random.randint(stream_key, (), max(1, total - bound), min(bound, total - 1) + 1)
        return jnp.stack([one, total - one])
    tallies = jnp.asarray(length_profile(count, total, bound, skew), jnp.int32)
    couples = (count - 1) // 2
    source_of, taker = tallies[1:1 + 2 * couples:2], tallies[2:2 + 2 * couples:2]
    margin = jnp.minimum(source_of - 1, bound - taker)
    passed = jax.random.randint(jax.random.fold_in(stream_key, 1), (couples,), 0, 1 << 20) % (margin + 1)
    tallies = tallies.at[1:1 + 2 * couples:2].set(source_of - passed).at[2:2 + 2 * couples:2].set(taker + passed)
    return tallies[jax.random.permutation(jax.random.fold_in(stream_key, 2), count)]


def gaussian(stream_key, extent, scale, reach, cuts=(), kind=jnp.bfloat16):
    values = scale * jax.random.normal(stream_key, extent, jnp.float32)
    if cuts:
        values = values * block_levels(stream_key, extent, cuts, -0.22, 0.18)
    return jnp.clip(values, -reach, reach).astype(kind)


def setup_inputs(seed: int = 0) -> dict:
    key_of = jax.random.split(jax.random.key(seed), 18)
    return {
        "hidden_in": gaussian(key_of[0], (TOKENS, D), 1.0, 6.0, ((0, 32),)),
        "seg_lengths": jax.vmap(lambda own: uneven_parts(own, SEGS, ROW_LEN, ROW_LEN // 4, 1))(jax.random.split(key_of[1], ROWS)).reshape((ROWS, SEGS)).astype(jnp.int32),
        "partner": draw_partner(jax.random.fold_in(key_of[17], 71), 0),
        "qkv_weight": gaussian(key_of[3], (LAYERS, D, 3, D), D ** -0.5, 0.1875, ((1, 8), (3, 4)), jnp.float32),
        "out_weight": gaussian(key_of[4], (LAYERS, D, D), (D * SEGS // ROW_LEN) ** -0.5, 2.0, ((1, 4), (2, 8)), jnp.float32),
        "up_weight": gaussian(key_of[5], (LAYERS, D, FF), D ** -0.5, 0.1875, ((1, 8), (2, 4)), jnp.float32),
        "down_weight": gaussian(key_of[6], (LAYERS, FF, D), FF ** -0.5, 0.09375, ((1, 4), (2, 8)), jnp.float32),
        "norm_params": draw_norm_params(jax.random.fold_in(key_of[17], 71), 0),
        "emb_weight": gaussian(key_of[8], (D, EMB), D ** -0.5, 0.1875, ((0, 8),), jnp.float32),
        "log_scale": jnp.clip(jax.random.uniform(key_of[9], (1,), jnp.float32, 2.5, 3.2), 2.5, 3.2),
        "qkv_moments": draw_qkv_moments(jax.random.fold_in(key_of[17], 71), 0),
        "out_moments": draw_out_moments(jax.random.fold_in(key_of[17], 71), 0),
        "up_moments": draw_up_moments(jax.random.fold_in(key_of[17], 71), 0),
        "down_moments": draw_down_moments(jax.random.fold_in(key_of[17], 71), 0),
        "norm_moments": draw_norm_moments(jax.random.fold_in(key_of[17], 71), 0),
        "emb_moments": draw_emb_moments(jax.random.fold_in(key_of[17], 71), 0),
        "scale_moments": draw_scale_moments(jax.random.fold_in(key_of[17], 71), 0),
    }


sharpness = 0.05
clip_limit = 1.0
best = lax.Precision.HIGHEST

@jax.custom_vjp
def low(v):
    return lax.optimization_barrier(v.astype(jnp.bfloat16)).astype(jnp.float32)

@jax.custom_vjp
def low_back(v):
    return v

def low_keep(v):
    return (low(v), None)

def low_pass(kept, grad):
    return (grad,)

def back_keep(v):
    return (v, None)

def back_low(kept, grad):
    return (low(grad),)
low.defvjp(low_keep, low_pass)
low_back.defvjp(back_keep, back_low)

def layer_norm(values, gain, bias):
    centered = values - lax.optimization_barrier(jnp.mean(values, axis=-1, keepdims=True))
    spread = lax.optimization_barrier(jnp.mean(centered * centered, axis=-1, keepdims=True))
    return centered * lax.rsqrt(spread + 1e-05) * gain + bias

def row_layout(lengths):
    ends = jnp.cumsum(lengths).astype(jnp.int32)
    places = jnp.arange(ROW_LEN, dtype=jnp.int32)
    after = places[:, None] >= ends[None, :]
    segment = lax.optimization_barrier(jnp.sum(after.astype(jnp.int32), axis=1)).astype(jnp.int32)
    starts = lax.optimization_barrier(jnp.sum(jnp.where(after, lengths[None, :], 0), axis=1)).astype(jnp.int32)
    return (segment, places - starts)

def rotary_tables(offsets):
    frequency = jnp.exp(jnp.arange(HEAD_DIM // 2, dtype=jnp.float32) * (-2.0 * math.log(10000.0) / HEAD_DIM))
    angles = offsets.astype(jnp.float32)[..., None] * frequency
    return (jnp.cos(angles), jnp.sin(angles))

def rotate(values, cosines, sines):
    half_dim = values.shape[-1] // 2
    leading = values[..., :half_dim]
    trailing = values[..., half_dim:]
    return jnp.concatenate([leading * cosines - trailing * sines, trailing * cosines + leading * sines], axis=-1)

def row_loss(embedded, log_scale, segment, lengths, partner):
    segment_count = lengths.shape[0]
    labels = jnp.arange(segment_count, dtype=jnp.int32)
    member = (segment[:, None] == labels[None, :]).astype(jnp.float32)
    scaling = jnp.exp(log_scale[0])
    columns = jnp.arange(embedded.shape[1], dtype=jnp.int32)
    allowed = labels[:, None] != labels[None, :]
    chosen = partner[:, None] == labels[None, :]
    counts_f = lengths.astype(jnp.float32)[:, None]
    result = jnp.zeros((), jnp.float32)
    for width_now in (EMB, EMB * 3 // 4, EMB // 2):
        keep_cols = (columns < width_now).astype(jnp.float32)
        masked = embedded * keep_cols[None, :]
        unit_rows = masked * lax.rsqrt(lax.optimization_barrier(jnp.sum(masked * masked, axis=1, keepdims=True)) + 1e-06)
        similar = jnp.dot(unit_rows, unit_rows.T, precision=best)
        soft_max = sharpness * jnp.log(jnp.dot(jnp.exp((similar - 1.0) / sharpness), member, precision=best)) + 1.0
        scores = jnp.dot(member.T, soft_max, precision=best) / counts_f
        logits = jnp.where(allowed, scaling * scores, -1e+30)
        highest = lax.optimization_barrier(jnp.max(logits, axis=1, keepdims=True))
        log_total = highest[:, 0] + jnp.log(lax.optimization_barrier(jnp.sum(jnp.exp(logits - highest), axis=1)))
        picked = lax.optimization_barrier(jnp.sum(jnp.where(chosen, logits, 0.0), axis=1))
        result = result + jnp.sum(log_total - picked)
    return result

def row_attention(operands):
    queries, key_rows, value_rows, segment = operands
    scores = low_back(jnp.einsum('qhd,khd->hqk', queries, key_rows, precision=best) * HEAD_DIM ** (-0.5))
    same = (segment[:, None] == segment[None, :])[None]
    scores = jnp.where(same, scores, -1e+30)
    highest = lax.optimization_barrier(jnp.max(scores, axis=-1, keepdims=True))
    weights_exp = jnp.exp(scores - highest)
    probs = low(weights_exp / lax.optimization_barrier(jnp.sum(weights_exp, axis=-1, keepdims=True)))
    return low(low_back(jnp.einsum('hqk,khd->qhd', probs, value_rows, precision=best)))

def forward(hidden, qkv_master, out_master, up_master, down_master, norm_master, emb_master, scale_log, segment, cosines, sines, seg_lengths, partner):
    qkv_low = low(qkv_master)
    out_low = low(out_master)
    up_low = low(up_master)
    down_low = low(down_master)
    norms = low(norm_master)
    emb_low = low(emb_master)
    heads_all = D // HEAD_DIM
    stream = hidden
    for layer_at in range(LAYERS):
        stream_low = low(stream)
        mixture = jnp.dot(stream_low, qkv_low[layer_at].reshape(D, 3 * D), precision=best).reshape(ROWS, ROW_LEN, 3, heads_all, HEAD_DIM)
        queries = low(rotate(low_back(mixture[:, :, 0]), cosines, sines))
        key_rows = low(rotate(low_back(mixture[:, :, 1]), cosines, sines))
        value_rows = low(low_back(mixture[:, :, 2]))
        attended = lax.map(jax.checkpoint(row_attention), (queries, key_rows, value_rows, segment))
        attn_out = low_back(jnp.dot(attended.reshape(TOKENS, D), out_low[layer_at], precision=best))
        normed = layer_norm(stream + attn_out, norms[layer_at, 0, 0], norms[layer_at, 0, 1])
        pre_act = low_back(jnp.dot(low(normed), up_low[layer_at], precision=best))
        activated = low(jax.nn.gelu(pre_act, approximate=False))
        ffn_out = low_back(jnp.dot(activated, down_low[layer_at], precision=best))
        stream = layer_norm(normed + ffn_out, norms[layer_at, 1, 0], norms[layer_at, 1, 1])
    embedded = low(low_back(jnp.dot(low(stream), emb_low, precision=best))).reshape(ROWS, ROW_LEN, EMB)
    losses = lax.map(lambda operands: row_loss(operands[0], scale_log, operands[1], operands[2], operands[3]), (embedded, segment, seg_lengths, partner))
    return (jnp.sum(losses), stream)

def adamw_update(master, moments, grad, factor, rate, step_f):
    scaled = grad * factor
    moment_one = 0.9 * moments[0] + 0.1 * scaled
    moment_two = 0.95 * moments[1] + 0.05 * scaled * scaled
    one_hat = moment_one / (1.0 - jnp.power(0.9, step_f))
    two_hat = moment_two / (1.0 - jnp.power(0.95, step_f))
    updated = master - rate * (one_hat / (jnp.sqrt(two_hat) + 1e-08) + 0.01 * master)
    return (updated, moment_one, moment_two)

def reference(hidden_in, seg_lengths, partner, qkv_weight, out_weight, up_weight, down_weight, norm_params, emb_weight, log_scale, qkv_moments, out_moments, up_moments, down_moments, norm_moments, emb_moments, scale_moments):
    segment, offsets = jax.vmap(row_layout)(seg_lengths)
    cosines, sines = rotary_tables(offsets)
    cosines = cosines[:, :, None, :]
    sines = sines[:, :, None, :]

    def wrapped(hidden, qkv_master, out_master, up_master, down_master, norm_master, emb_master, scale_log):
        return forward(hidden, qkv_master, out_master, up_master, down_master, norm_master, emb_master, scale_log, segment, cosines, sines, seg_lengths, partner)
    loss_value, backward_fn, hidden_out = jax.vjp(wrapped, hidden_in.astype(jnp.float32), qkv_weight, out_weight, up_weight, down_weight, norm_params, emb_weight, log_scale, has_aux=True)
    grads = backward_fn(jnp.ones((), jnp.float32))
    hidden_grad = grads[0]
    weight_grads = grads[1:]
    squares = jnp.zeros((), jnp.float32)
    for piece in weight_grads:
        squares = squares + jnp.sum(piece * piece)
    norm_value = jnp.sqrt(squares + 1e-06)
    factor = clip_limit / jnp.maximum(norm_value, clip_limit)
    step_f = jnp.asarray(STEP, jnp.float32)
    qkv_new, qkv_first, qkv_second = adamw_update(qkv_weight, qkv_moments, weight_grads[0], factor, D ** (-0.5), step_f)
    out_new, out_first, out_second = adamw_update(out_weight, out_moments, weight_grads[1], factor, (D * SEGS // ROW_LEN) ** (-0.5), step_f)
    up_new, up_first, up_second = adamw_update(up_weight, up_moments, weight_grads[2], factor, D ** (-0.5), step_f)
    down_new, down_first, down_second = adamw_update(down_weight, down_moments, weight_grads[3], factor, FF ** (-0.5), step_f)
    norm_new, norm_first, norm_second = adamw_update(norm_params, norm_moments, weight_grads[4], factor, 0.5, step_f)
    emb_new, emb_first, emb_second = adamw_update(emb_weight, emb_moments, weight_grads[5], factor, D ** (-0.5), step_f)
    scale_new, scale_first, scale_second = adamw_update(log_scale, scale_moments, weight_grads[6], factor, 1.0, step_f)
    return (hidden_out, hidden_grad, loss_value.reshape(1), norm_value.reshape(1), qkv_new, qkv_first, qkv_second, out_new, out_first, out_second, up_new, up_first, up_second, down_new, down_first, down_second, norm_new, norm_first, norm_second, emb_new, emb_first, emb_second, scale_new, scale_first, scale_second)
```

```python
import functools
import math

import jax
import jax.numpy as jnp
from jax import lax
from jax.experimental import pallas as pl
from jax.experimental.pallas import tpu as pltpu
from jax.sharding import PartitionSpec as P

D = 1024
HEAD_DIM = 64
FF = 4096
EMB = 128
LAYERS = 2
STEP = 5
ROW_LEN = 1024
SEGS = 8

BLK = 256
HALF = 512
WIDE = 256
HID = 1024
PAIR = 128
PAIRS = WIDE // PAIR
MIB = 1 << 20
COST = 1

f32 = jnp.float32
bf16 = jnp.bfloat16
best = lax.Precision.HIGHEST
sharpness = 0.05
clip_limit = 1.0

OUT_AT = 3 * WIDE


def dot_nn(left, right):
    return lax.dot_general(left, right, (((1,), (0,)), ((), ())), preferred_element_type=f32)


def dot_nt(left, right):
    return lax.dot_general(left, right, (((1,), (1,)), ((), ())), preferred_element_type=f32)


def dot_tn(left, right):
    return lax.dot_general(left, right, (((0,), (0,)), ((), ())), preferred_element_type=f32)


def whole(shape):
    return pl.BlockSpec(shape, lambda *_: (0,) * len(shape))


def call(kernel, args, in_specs, outs, out_specs=None, grid=(1,), scratch=(), flops=0, vmem=32, alias=None,
         keep=(), after=None, far=()):
    out_shape = [
        pltpu.HBM(s, d) if i in keep else jax.ShapeDtypeStruct(s, d) for i, (s, d) in enumerate(outs)
    ]
    if out_specs is None:
        out_specs = [whole(s) for s, _ in outs]
    args = [pltpu.with_memory_space_constraint(a, pltpu.HBM) if i in far else a for i, a in enumerate(args)]
    in_specs = list(in_specs)
    moved = sum(math.prod(a.shape) * a.dtype.itemsize for a in args if a.size < 3 * MIB)
    moved += sum(math.prod(s) * jnp.dtype(d).itemsize for s, d in outs)
    body_fn = kernel
    if after is not None:
        count = len(args)
        args = args + [after]
        in_specs = in_specs + [pl.BlockSpec(memory_space=pl.ANY)]

        def body_fn(*refs):
            kernel(*refs[:count], *refs[count + 1 :])

    return pl.pallas_call(
        body_fn,
        grid=grid,
        in_specs=in_specs,
        out_specs=out_specs,
        out_shape=out_shape,
        scratch_shapes=list(scratch),
        input_output_aliases=alias or {},
        compiler_params=pltpu.CompilerParams(
            dimension_semantics=("arbitrary",) * len(grid), vmem_limit_bytes=vmem * MIB
        ),
        cost_estimate=pl.CostEstimate(flops=int(flops * COST), bytes_accessed=int(moved * COST), transcendentals=0),
    )(*args)


def smem():
    return pl.BlockSpec(memory_space=pltpu.SMEM)


def halves(values):
    high = values.astype(bf16)
    return high, (values - high.astype(f32)).astype(bf16)


def norm_fwd_kernel(row, with_sums, *refs):
    if with_sums:
        x_ref, s_ref, r_ref, n_ref, h_ref, hb_ref, z_ref = refs
        v = x_ref[...].astype(f32) + (s_ref[...].astype(f32) + r_ref[...].astype(f32))
    else:
        x_ref, n_ref, h_ref, hb_ref, z_ref = refs
        v = x_ref[...].astype(f32)
    cen = v - jnp.mean(v, axis=1, keepdims=True)
    var = jnp.mean(cen * cen, axis=1, keepdims=True)
    rstd = lax.rsqrt(var + 1e-05)
    z = cen * rstd
    h = z * n_ref[row : row + 1, :] + n_ref[row + 1 : row + 2, :]
    h_ref[...] = h
    hb_ref[...] = h.astype(bf16)
    z_ref[:, 0:D] = z.astype(bf16)
    high, rest = halves(rstd)
    lane = lax.broadcasted_iota(jnp.int32, (BLK, PAIR), 1)
    z_ref[:, D:] = jnp.where(lane < 1, high.astype(f32), rest.astype(f32)).astype(bf16)


def norm_fwd(row, x, s, r, nrm):
    blk = whole((BLK, D))
    return call(
        functools.partial(norm_fwd_kernel, row, True),
        (x, s, r, nrm),
        [blk, blk, blk, whole(nrm.shape)],
        [((BLK, D), f32), ((BLK, D), bf16), ((BLK, D + PAIR), bf16)],
        flops=BLK * D * 10,
        keep=(2,),
    )


def norm_bwd_kernel(row, with_sums, *refs):
    if with_sums:
        d_ref, s_ref, r_ref, z_ref, n_ref, o_ref, ob_ref, g_ref = refs
        dy = d_ref[...] + (s_ref[...].astype(f32) + r_ref[...].astype(f32))
    else:
        d_ref, z_ref, n_ref, o_ref, ob_ref, g_ref = refs
        dy = d_ref[...]
    z = z_ref[:, 0:D].astype(f32)
    rstd = z_ref[:, D : D + 1].astype(f32) + z_ref[:, D + 1 : D + 2].astype(f32)
    dz = dy * n_ref[row : row + 1, :]
    m1 = jnp.mean(dz, axis=1, keepdims=True)
    m2 = jnp.mean(dz * z, axis=1, keepdims=True)
    dr = (dz - m1 - z * m2) * rstd
    o_ref[...] = dr
    ob_ref[...] = dr.astype(bf16)
    g_ref[...] = jnp.concatenate(
        [jnp.sum(dy * z, axis=0, keepdims=True), jnp.sum(dy, axis=0, keepdims=True), jnp.zeros((6, D), f32)],
        axis=0,
    )


def norm_bwd(row, d, sums, z, nrm):
    blk = whole((BLK, D))
    args = (d,) + tuple(sums) + (z, nrm)
    return call(
        functools.partial(norm_bwd_kernel, row, len(sums) > 0),
        args,
        [blk] * (1 + len(sums)) + [whole((BLK, D + PAIR)), whole(nrm.shape)],
        [((BLK, D), f32), ((BLK, D), bf16), ((8, D), f32)],
        flops=BLK * D * 14,
        far=(1 + len(sums),),
    )


def rope_lanes(values, cosines, sines):
    lane = lax.broadcasted_iota(jnp.int32, values.shape, 1)
    low = (lane & (HEAD_DIM - 1)) < HEAD_DIM // 2
    swapped = jnp.where(
        low, pltpu.roll(values, PAIR - HEAD_DIM // 2, 1), pltpu.roll(values, HEAD_DIM // 2, 1)
    )
    return values * cosines + swapped * sines


def qkv_kernel(xo_ref, xs_ref, w_ref, c_ref, s_ref, m_ref):
    for at, x_ref in enumerate((xo_ref, xs_ref)):
        rows = slice(at * BLK, (at + 1) * BLK)
        mix = dot_nn(x_ref[...], w_ref[...])
        cosines, sines = c_ref[rows, :], s_ref[rows, :]
        for p in range(PAIRS):
            lanes = slice(p * PAIR, (p + 1) * PAIR)
            q = rope_lanes(mix[:, p * PAIR : (p + 1) * PAIR], cosines, sines).astype(bf16)
            m_ref[rows, lanes] = q * HEAD_DIM ** (-0.5)
            lanes = slice(WIDE + p * PAIR, WIDE + (p + 1) * PAIR)
            m_ref[rows, lanes] = rope_lanes(mix[:, lanes], cosines, sines).astype(bf16)
        m_ref[rows, 2 * WIDE :] = mix[:, 2 * WIDE :].astype(bf16)


def qkv_project(x_own, x_sib, weights, cosines, sines, at):
    blk = whole((BLK, D))
    tab = pl.BlockSpec((HALF, PAIR), lambda *_: (at, 0))
    return call(
        qkv_kernel,
        (x_own, x_sib, weights, cosines, sines),
        [blk, blk, pl.BlockSpec((D, 3 * WIDE), lambda *_: (0, 0)), tab, tab],
        [((HALF, 3 * WIDE), bf16)],
        flops=2 * HALF * D * 3 * WIDE,
        keep=(0,),
    )[0]


def near_places(core, at):
    if at == 0:
        return 1 - core, core
    return core, 1 - core


def attend_kernel(at, core_ref, m_ref, mo_ref, sc_ref, sco_ref, sr_ref, w_ref, o_ref, l_ref, own_ref, send_ref):
    q_ref, k_ref, v_ref = [m_ref.at[:, i * WIDE : (i + 1) * WIDE] for i in range(3)]
    ko_ref, vo_ref = [mo_ref.at[:, i * WIDE : (i + 1) * WIDE] for i in (1, 2)]
    near, cross = near_places(core_ref[0], at)
    cross_rows = pl.ds(pl.multiple_of(cross * BLK, BLK), BLK)
    row_at = lax.broadcasted_iota(jnp.int32, (PAIR, BLK), 0)
    lane_at = lax.broadcasted_iota(jnp.int32, (BLK, PAIR), 1)
    seg_main = sc_ref[...]
    seg_main = jnp.concatenate([seg_main, seg_main], axis=1)
    seg_cross = sco_ref[cross_rows, :]
    seg_cross = jnp.concatenate([seg_cross, seg_cross], axis=1)
    l_ref[...] = jnp.zeros(l_ref.shape, f32)
    for is_near in (False, True):
        place = near if is_near else 1 - near
        start = pl.multiple_of(place * BLK, BLK)
        rows = pl.ds(start, BLK)
        seg_q = sr_ref[0:1, rows]
        bias = jnp.where(seg_main == seg_q, 0.0, -1e30)
        if is_near:
            bias_cross = jnp.where(seg_cross == seg_q, 0.0, -1e30)
        for p in range(PAIRS):
            lanes = slice(p * PAIR, (p + 1) * PAIR)
            keys = k_ref[:, lanes]
            values_t = v_ref[:, lanes].T
            queries = q_ref[rows, lanes]
            if is_near:
                keys_cross = ko_ref[cross_rows, lanes]
                values_cross_t = vo_ref[cross_rows, lanes].T
            parts = []
            for h in range(2):
                q = jnp.where((lane_at >= HEAD_DIM) == (h == 1), queries, jnp.zeros_like(queries))
                scores = dot_nt(keys, q) + bias
                top = jnp.max(scores, axis=0, keepdims=True)
                if is_near:
                    scores_cross = dot_nt(keys_cross, q) + bias_cross
                    top = jnp.maximum(top, jnp.max(scores_cross, axis=0, keepdims=True))
                e = jnp.exp(scores - top)
                total = jnp.sum(e, axis=0, keepdims=True)
                mixed = dot_nn(values_t, e.astype(bf16))
                if is_near:
                    e = jnp.exp(scores_cross - top)
                    total = total + jnp.sum(e, axis=0, keepdims=True)
                    mixed = mixed + dot_nn(values_cross_t, e.astype(bf16))
                parts.append(mixed / total)
                head = 2 * p + h
                l_ref[head : head + 1, rows] = top + jnp.log(total)
            both = jnp.where(row_at < HEAD_DIM, parts[0], parts[1])
            o_ref[rows, lanes] = both.T.astype(bf16)
    own_ref[...] = dot_nt(o_ref[0:BLK, :], w_ref[...]).astype(bf16)
    send_ref[...] = dot_nt(o_ref[BLK:HALF, :], w_ref[...]).astype(bf16)


def attend(at, core, qkv, qkv_other, seg_col, seg_row, weights, after):
    mix = whole((HALF, 3 * WIDE))
    return call(
        functools.partial(attend_kernel, at),
        (core, qkv, qkv_other, seg_col, seg_col, seg_row, weights),
        [
            smem(), mix, mix,
            pl.BlockSpec((HALF, PAIR), lambda *_: (at, 0)),
            pl.BlockSpec((HALF, PAIR), lambda *_: (1 - at, 0)),
            pl.BlockSpec((8, HALF), lambda *_: (0, at)),
            pl.BlockSpec((D, WIDE), lambda *_: (0, OUT_AT // WIDE)),
        ],
        [((HALF, WIDE), bf16), ((8, HALF), f32), ((BLK, D), bf16), ((BLK, D), bf16)],
        flops=4 * 4 * 5 * BLK * BLK * PAIR + 2 * HALF * WIDE * D,
        far=(1, 2),
        keep=(0, 1),
        after=after,
    )


def attend_back_kernel(core_ref, d0o, d0s, d1o, d1s, w_ref, mix0, mix1, o0, o1, l0, l1,
                       sc_ref, sr_ref, c_ref, s_ref, m0_ref, m1_ref,
                       dout_ref, dk_ref, dv_ref, dq_ref):
    for i, d in enumerate((d0o, d0s, d1o, d1s)):
        dout_ref[i // 2, (i % 2) * BLK : (i % 2 + 1) * BLK, :] = dot_nn(d[...], w_ref[...]).astype(bf16)
    dk_ref[...] = jnp.zeros(dk_ref.shape, f32)
    dv_ref[...] = jnp.zeros(dv_ref.shape, f32)
    row_at = lax.broadcasted_iota(jnp.int32, (PAIR, 1), 0)
    lane_at = lax.broadcasted_iota(jnp.int32, (1, PAIR), 1)
    scaling = HEAD_DIM ** (-0.5)
    q_refs, k_refs, v_refs = [
        [m.at[:, i * WIDE : (i + 1) * WIDE] for m in (mix0, mix1)] for i in range(3)
    ]
    o_refs, l_refs = (o0, o1), (l0, l1)
    for at in range(2):
        near, cross = near_places(core_ref[0], at)
        cross_rows = pl.ds(pl.multiple_of(cross * BLK, BLK), BLK)
        cross_full = pl.ds(pl.multiple_of((1 - at) * HALF + cross * BLK, BLK), BLK)
        seg_main = sc_ref[at * HALF : (at + 1) * HALF, :]
        seg_main = jnp.concatenate([seg_main, seg_main], axis=1)
        seg_cross = sc_ref[cross_full, :]
        seg_cross = jnp.concatenate([seg_cross, seg_cross], axis=1)
        for is_near in (False, True):
            place = near if is_near else 1 - near
            rows = pl.ds(pl.multiple_of(place * BLK, BLK), BLK)
            seg_q = sr_ref[0:1, pl.ds(pl.multiple_of(at * HALF + place * BLK, BLK), BLK)]
            bias = jnp.where(seg_main == seg_q, 0.0, -1e30)
            if is_near:
                bias_cross = jnp.where(seg_cross == seg_q, 0.0, -1e30)
            for p in range(PAIRS):
                lanes = slice(p * PAIR, (p + 1) * PAIR)
                keys, values = k_refs[at][:, lanes], v_refs[at][:, lanes]
                keys_t = keys.T
                queries, douts = q_refs[at][rows, lanes], dout_ref[at, rows, lanes]
                if is_near:
                    keys_cross = k_refs[1 - at][cross_rows, lanes]
                    values_cross = v_refs[1 - at][cross_rows, lanes]
                    keys_cross_t = keys_cross.T
                products = (douts.astype(f32) * o_refs[at][rows, lanes].astype(f32)).T
                dq_t = jnp.zeros((PAIR, BLK), f32)
                for h in range(2):
                    in_lanes = (lane_at >= HEAD_DIM) == (h == 1)
                    in_rows = (row_at >= HEAD_DIM) == (h == 1)
                    q = jnp.where(in_lanes, queries, jnp.zeros_like(queries))
                    d = jnp.where(in_lanes, douts, jnp.zeros_like(douts))
                    delta = jnp.sum(products[h * HEAD_DIM : (h + 1) * HEAD_DIM, :], axis=0, keepdims=True)
                    lse = l_refs[at][2 * p + h : 2 * p + h + 1, rows]
                    kt = jnp.where(in_rows, keys_t, jnp.zeros_like(keys_t))
                    probs = jnp.exp(dot_nt(keys, q) + bias - lse)
                    dscores = (probs * (dot_nt(values, d) - delta)).astype(bf16)
                    dv_ref[at, :, lanes] += dot_nn(probs.astype(bf16), d)
                    dk_ref[at, :, lanes] += dot_nn(dscores, q)
                    dq_t = dq_t + dot_nn(kt, dscores)
                    if is_near:
                        kt = jnp.where(in_rows, keys_cross_t, jnp.zeros_like(keys_cross_t))
                        probs = jnp.exp(dot_nt(keys_cross, q) + bias_cross - lse)
                        dscores = (probs * (dot_nt(values_cross, d) - delta)).astype(bf16)
                        dv_ref[1 - at, cross_rows, lanes] += dot_nn(probs.astype(bf16), d)
                        dk_ref[1 - at, cross_rows, lanes] += dot_nn(dscores, q)
                        dq_t = dq_t + dot_nn(kt, dscores)
                dq_ref[at, rows, lanes] = dq_t.T * scaling
    for at, m_ref in enumerate((m0_ref, m1_ref)):
        rows = slice(at * HALF, (at + 1) * HALF)
        cosines, sines = c_ref[rows, :], -s_ref[rows, :]
        for p in range(PAIRS):
            lanes = slice(p * PAIR, (p + 1) * PAIR)
            m_ref[:, p * PAIR : (p + 1) * PAIR] = rope_lanes(dq_ref[at, :, lanes], cosines, sines).astype(bf16)
            m_ref[:, WIDE + p * PAIR : WIDE + (p + 1) * PAIR] = rope_lanes(
                dk_ref[at, :, lanes], cosines, sines
            ).astype(bf16)
        m_ref[:, 2 * WIDE :] = dv_ref[at].astype(bf16)


def attend_back(core, dblocks, weights, qkv_a, qkv_b, o_a, o_b, l_a, l_b, seg_col, seg_row, cosines, sines):
    blk, half, low, mix = whole((BLK, D)), whole((HALF, WIDE)), whole((8, HALF)), whole((HALF, 3 * WIDE))
    tab = whole((ROW_LEN, PAIR))
    return call(
        attend_back_kernel,
        (core, *dblocks, weights, qkv_a, qkv_b, o_a, o_b, l_a, l_b, seg_col, seg_row, cosines, sines),
        [smem(), blk, blk, blk, blk, pl.BlockSpec((D, WIDE), lambda *_: (0, OUT_AT // WIDE))]
        + [mix, mix, half, half]
        + [low, low, tab, whole((8, ROW_LEN)), tab, tab],
        [((HALF, 3 * WIDE), bf16)] * 2,
        scratch=[
            pltpu.VMEM((2, HALF, WIDE), bf16),
            pltpu.VMEM((2, HALF, WIDE), f32),
            pltpu.VMEM((2, HALF, WIDE), f32),
            pltpu.VMEM((2, HALF, WIDE), f32),
        ],
        flops=10 * 4 * 10 * BLK * BLK * PAIR + 2 * ROW_LEN * WIDE * D,
        far=(6, 7, 8, 9, 10, 11),
    )


def spread_kernel(m_ref, w_ref, own_ref, send_ref):
    own_ref[...] = dot_nt(m_ref[0:BLK, :], w_ref[...]).astype(bf16)
    send_ref[...] = dot_nt(m_ref[BLK:HALF, :], w_ref[...]).astype(bf16)


def qkv_back(dmix, weights, after):
    return call(
        spread_kernel,
        (dmix, weights),
        [whole(dmix.shape), pl.BlockSpec((D, 3 * WIDE), lambda *_: (0, 0))],
        [((BLK, D), bf16)] * 2,
        flops=2 * HALF * D * 3 * WIDE,
        after=after,
    )


TILE = 256
TILES = HID // TILE


def gelu_pair(u):
    half = jnp.exp(u * u * -0.5)
    t = 1.0 / (1.0 + (0.3275911 * 0.5 ** 0.5) * jnp.abs(u))
    poly = t * (
        0.5 * 0.254829592
        + t * (0.5 * -0.284496736 + t * (0.5 * 1.421413741 + t * (0.5 * -1.453152027 + t * (0.5 * 1.061405429))))
    )
    tail = poly * half
    phi = jnp.where(u >= 0.0, 1.0 - tail, tail)
    return u * phi, phi + u * half * (1.0 / math.sqrt(2.0 * math.pi))


def mlp_kernel(ho_ref, hs_ref, up_ref, down_ref, zg_ref, own_ref, send_ref):
    for at, (h_ref, p_ref) in enumerate(((ho_ref, own_ref), (hs_ref, send_ref))):
        rows = slice(at * BLK, (at + 1) * BLK)
        value, slope = gelu_pair(dot_nn(h_ref[...], up_ref[...]))
        z = value.astype(bf16)
        zg_ref[rows, 0:HID] = z
        zg_ref[rows, HID:] = slope.astype(bf16)
        p_ref[...] = dot_nt(z, down_ref[...]).astype(bf16)


def mlp(h_own, h_sib, weights, after):
    blk = whole((BLK, D))
    array, first = weights
    return call(
        mlp_kernel,
        (h_own, h_sib, array, array),
        [
            blk, blk,
            pl.BlockSpec((D, HID), lambda *_: (0, first)),
            pl.BlockSpec((D, HID), lambda *_: (0, first + 1)),
        ],
        [((HALF, 2 * HID), bf16), ((BLK, D), bf16), ((BLK, D), bf16)],
        flops=4 * HALF * D * HID,
        keep=(0,),
        after=after,
    )


def mlp_back_kernel(do_ref, ds_ref, g_ref, up_ref, down_ref, du_ref, own_ref, send_ref):
    for at, (d_ref, p_ref) in enumerate(((do_ref, own_ref), (ds_ref, send_ref))):
        rows = slice(at * BLK, (at + 1) * BLK)
        du = (dot_nn(d_ref[...], down_ref[...]) * g_ref[rows, :].astype(f32)).astype(bf16)
        du_ref[rows, :] = du
        p_ref[...] = dot_nt(du, up_ref[...]).astype(bf16)


def mlp_back(d_own, d_sib, zg, weights, after):
    blk = whole((BLK, D))
    array, first = weights
    return call(
        mlp_back_kernel,
        (d_own, d_sib, zg, array, array),
        [
            blk, blk,
            pl.BlockSpec((HALF, HID), lambda *_: (0, 1)),
            pl.BlockSpec((D, HID), lambda *_: (0, first)),
            pl.BlockSpec((D, HID), lambda *_: (0, first + 1)),
        ],
        [((HALF, HID), bf16), ((BLK, D), bf16), ((BLK, D), bf16)],
        flops=4 * HALF * D * HID,
        far=(2,),
        after=after,
    )


def turn_into(t_ref, x_refs):
    for i, x in enumerate(x_refs):
        t_ref[:, i * BLK : (i + 1) * BLK] = x[...].T


def grad_tile(t_ref, y_refs):
    first, second = y_refs
    return (dot_nn(t_ref[:, 0:HALF], first[...]) + dot_nn(t_ref[:, HALF:], second[...])).astype(bf16)


def mlp_grad_kernel(x0, x1, x2, x3, d0, d1, d2, d3, u0, u1, z0, z1, g_ref, t_ref):
    step = pl.program_id(0)

    @pl.when(step == 0)
    def _():
        turn_into(t_ref, (x0, x1, x2, x3))

    @pl.when(step == HID // HALF)
    def _():
        turn_into(t_ref, (d0, d1, d2, d3))

    @pl.when(step < HID // HALF)
    def _():
        g_ref[...] = grad_tile(t_ref, (u0, u1))

    @pl.when(step >= HID // HALF)
    def _():
        g_ref[...] = grad_tile(t_ref, (z0, z1))


def mlp_grads(hidden, dblocks, dus, zs, after):
    blk = whole((BLK, D))
    tiles = HID // HALF
    first = pl.BlockSpec((HALF, HALF), lambda t: (0, jnp.minimum(t, tiles - 1)))
    second = pl.BlockSpec((HALF, HALF), lambda t: (0, jnp.maximum(t - tiles, 0)))
    return call(
        mlp_grad_kernel,
        (*hidden, *dblocks, *dus, *zs),
        [blk] * 8 + [first] * 2 + [second] * 2,
        [((D, 2 * HID), bf16)],
        out_specs=[pl.BlockSpec((D, HALF), lambda t: (0, t))],
        grid=(2 * tiles,),
        scratch=[pltpu.VMEM((D, ROW_LEN), bf16)],
        flops=4 * ROW_LEN * D * HID,
        keep=(0,),
        after=after,
    )[0]


def attn_grad_kernel(with_small, x0, x1, x2, x3, d0, d1, d2, d3, m0, m1, o0, o1, *refs):
    g_ref, t_ref = refs[-2:]
    step = pl.program_id(0)

    @pl.when(step == 0)
    def _():
        turn_into(t_ref, (x0, x1, x2, x3))

    @pl.when(step == 3)
    def _():
        turn_into(t_ref, (d0, d1, d2, d3))

    @pl.when(step < 3)
    def _():
        g_ref[...] = grad_tile(t_ref, (m0, m1))

    @pl.when(step == 3)
    def _():
        g_ref[...] = grad_tile(t_ref, (o0, o1))

    if with_small:

        @pl.when(step == 4)
        def _():
            g_ref[...] = refs[0][...]


def attn_grads(streams, dblocks, dmixes, outs, after, small=None):
    blk = whole((BLK, D))
    first = pl.BlockSpec((HALF, WIDE), lambda t: (0, jnp.minimum(t, 2)))
    args = (*streams, *dblocks, *dmixes, *outs) + (() if small is None else (small,))
    specs = [blk] * 8 + [first] * 2 + [whole((HALF, WIDE))] * 2
    specs += [] if small is None else [whole((D, WIDE))]
    steps = 4 if small is None else 5
    return call(
        functools.partial(attn_grad_kernel, small is not None),
        args,
        specs,
        [((D, steps * WIDE), bf16)],
        out_specs=[pl.BlockSpec((D, WIDE), lambda t: (0, t))],
        grid=(steps,),
        scratch=[pltpu.VMEM((D, ROW_LEN), bf16)],
        flops=2 * ROW_LEN * D * 4 * WIDE,
        after=after,
    )[0]


def loss_kernel(ls_ref, e_ref, seg_ref, segr_ref, len_ref, par_ref, x0_ref, x1_ref, we_ref,
                dx0_ref, dx1_ref, ge_ref, out_ref, sim_ref, b_ref, ll_ref, de_ref):
    tokens = ROW_LEN
    mine = HALF
    width_blk = BLK
    emb = e_ref[...].astype(f32)
    emb_t = emb.T
    lanes = lax.broadcasted_iota(jnp.int32, (tokens, PAIR), 1)
    label_col = lanes.astype(f32)
    member = (seg_ref[...] == label_col).astype(bf16)
    rows16 = lax.broadcasted_iota(jnp.int32, (16, tokens), 0).astype(f32)
    member_t = (jnp.broadcast_to(segr_ref[0:1, :], (16, tokens)) == rows16).astype(bf16)
    scale = jnp.exp(ls_ref[0])
    cls = lax.broadcasted_iota(jnp.int32, (16, PAIR), 0)
    seg = lax.broadcasted_iota(jnp.int32, (16, PAIR), 1)
    real = (cls < SEGS) & (seg < SEGS)
    allowed = (cls != seg) & real
    lengths = len_ref[0:1, :]
    chosen = (cls.astype(f32) == par_ref[0:1, :]) & real
    loss = jnp.zeros((1, PAIR), f32)
    dscale = jnp.zeros((1, PAIR), f32)
    de_ref[...] = jnp.zeros(de_ref.shape, f32)
    for width in (EMB, EMB * 3 // 4, EMB // 2):
        kept = jnp.where(lanes < width, emb, 0.0)
        r_col = lax.rsqrt(jnp.sum(kept * kept, axis=1, keepdims=True) + 1e-06)
        kept_low = kept.astype(bf16)
        row_of = lax.broadcasted_iota(jnp.int32, (PAIR, tokens), 0)
        kept_t = jnp.where(row_of < width, emb_t, 0.0)
        r_row = lax.rsqrt(jnp.sum(kept_t * kept_t, axis=0, keepdims=True) + 1e-06)
        b_ref[16:24, :] = jnp.broadcast_to(r_row, (8, tokens))

        def sims(i, carry):
            at = pl.multiple_of(i * width_blk, width_blk)
            cols = pl.ds(at, width_blk)
            other = jnp.where(lanes[0:width_blk, :] < width, e_ref[cols, :], jnp.zeros((width_blk, PAIR), bf16))
            near = dot_nt(kept_low, other)
            expo = jnp.exp(near * r_col * (b_ref[16:17, cols] * (1.0 / sharpness)) - 1.0 / sharpness)
            sim_ref[:, cols] = expo
            ll_ref[:, cols] = dot_nn(member_t, expo.astype(bf16))
            return carry

        lax.fori_loop(0, tokens // width_blk, sims, 0)
        totals = ll_ref[...]
        sum_rows = lax.broadcasted_iota(jnp.int32, totals.shape, 0)
        totals = jnp.where(sum_rows < SEGS, totals, 1.0)
        soft = sharpness * jnp.log(totals) + 1.0
        score = jnp.dot(soft, member.astype(f32), precision=best, preferred_element_type=f32) / lengths
        logits = jnp.where(allowed, scale * score, -1e30)
        top = jnp.max(logits, axis=0, keepdims=True)
        powers = jnp.exp(logits - top)
        summed = jnp.sum(powers, axis=0, keepdims=True)
        picked = jnp.sum(jnp.where(chosen, logits, 0.0), axis=0, keepdims=True)
        live = seg[0:1, :] < SEGS
        loss = loss + jnp.where(live, top + jnp.log(summed) - picked, 0.0)
        dlogit = jnp.where(allowed, powers / summed - chosen.astype(f32), 0.0)
        dscale = dscale + jnp.sum(dlogit * jnp.where(allowed, logits, 0.0), axis=0, keepdims=True)
        dscore = dlogit * scale / lengths
        dsoft = jnp.dot(dscore, jnp.concatenate([member_t.astype(f32), jnp.zeros((PAIR - 16, tokens), f32)], axis=0),
                        precision=best, preferred_element_type=f32)
        coef = dsoft / totals
        b_ref[0:16, :] = coef
        coef_high, coef_rest = halves(coef)
        left = jnp.concatenate([member_t, member_t, coef_high, coef_rest], axis=0)
        keep_t = kept_t.astype(bf16)

        def pulls(i, carry):
            at = pl.multiple_of(i * width_blk, width_blk)
            cols = pl.ds(at, width_blk)
            here_high, here_rest = halves(b_ref[0:16, cols])
            member_here = (
                jnp.broadcast_to(segr_ref[0:1, cols], (16, width_blk)) == rows16[:, 0:width_blk]
            ).astype(bf16)
            right = jnp.concatenate([here_high, here_rest, member_here, member_here], axis=0)
            pull = dot_tn(left, right) * sim_ref[:, cols] * r_col
            high, rest = halves(pull)
            de = dot_nn(keep_t, high) + dot_nn(keep_t, rest)
            r_here = b_ref[16:17, cols]
            e_here = jnp.where(lanes[0:width_blk, :] < width, e_ref[cols, :].astype(f32), 0.0).T
            along = jnp.sum(e_here * de, axis=0, keepdims=True)
            de_ref[:, cols] += r_here * de - (r_here * r_here * r_here * along) * e_here
            return carry

        lax.fori_loop(0, mine // width_blk, pulls, 0)
    de = de_ref[...].T.astype(bf16)
    dx0_ref[...] = dot_nt(de[0:BLK, :], we_ref[...])
    dx1_ref[...] = dot_nt(de[BLK:HALF, :], we_ref[...])
    ge_ref[...] = dot_tn(x0_ref[...], de[0:BLK, :]) + dot_tn(x1_ref[...], de[BLK:HALF, :])
    out_ref[...] = jnp.concatenate([loss, dscale, jnp.zeros((6, PAIR), f32)], axis=0)


def loss_and_grads(log_scale, emb, seg_col, seg_row, lengths, partner, x0, x1, w_emb):
    blk = whole((BLK, D))
    return call(
        loss_kernel,
        (log_scale, emb, seg_col, seg_row, lengths, partner, x0, x1, w_emb),
        [
            smem(), whole((ROW_LEN, EMB)), whole((ROW_LEN, PAIR)), whole((8, ROW_LEN)),
            whole((8, PAIR)), whole((8, PAIR)), blk, blk, whole((D, EMB)),
        ],
        [((BLK, D), f32), ((BLK, D), f32), ((D, EMB), f32), ((8, PAIR), f32)],
        scratch=[
            pltpu.VMEM((ROW_LEN, ROW_LEN), f32),
            pltpu.VMEM((24, ROW_LEN), f32),
            pltpu.VMEM((16, ROW_LEN), f32),
            pltpu.VMEM((EMB, HALF), f32),
        ],
        flops=20 * ROW_LEN * ROW_LEN * EMB,
    )


def row_layout(lengths):
    ends = jnp.cumsum(lengths)
    places = jnp.arange(ROW_LEN, dtype=jnp.int32)
    after = places[:, None] >= ends[None, :]
    segment = jnp.sum(after.astype(jnp.int32), axis=1)
    starts = jnp.sum(jnp.where(after, lengths[None, :], 0), axis=1)
    return (segment, places - starts)


def adamw_update(master, moments, grad, factor, rate, step_f):
    scaled = grad * factor
    moment_one = 0.9 * moments[0] + 0.1 * scaled
    moment_two = 0.95 * moments[1] + 0.05 * scaled * scaled
    one_hat = moment_one / (1.0 - jnp.power(0.9, step_f))
    two_hat = moment_two / (1.0 - jnp.power(0.95, step_f))
    updated = master - rate * (one_hat / (jnp.sqrt(two_hat) + 1e-08) + 0.01 * master)
    return (updated, moment_one, moment_two)


def adam_kernel(rate, turned, k_ref, w_ref, m_ref, v_ref, g0_ref, g1_ref, wo_ref, mo_ref, vo_ref):
    grad = jnp.where(pl.program_id(0) == 0, g0_ref[...].astype(f32), g1_ref[...].astype(f32))
    if turned:
        grad = grad.T
    grad = (grad * k_ref[0]).reshape(w_ref.shape)
    one = 0.9 * m_ref[...].reshape(w_ref.shape) + 0.1 * grad
    two = 0.95 * v_ref[...].reshape(w_ref.shape) + 0.05 * grad * grad
    w = w_ref[...]
    one_hat = one * (1.0 / (1.0 - 0.9 ** STEP))
    two_hat = two * (1.0 / (1.0 - 0.95 ** STEP))
    wo_ref[...] = w - rate * (one_hat / (jnp.sqrt(two_hat) + 1e-08) + 0.01 * w)
    mo_ref[...] = one
    vo_ref[...] = two


def adam_step(factor, master, moments, grads, tiles, block, where_of, grad_block, grad_at, rate, turned=False):
    spec = pl.BlockSpec((1,) + block, lambda l, t: (l,) + where_of(t))
    first = pl.BlockSpec((1, 1) + block, lambda l, t: (0, l) + where_of(t))
    second = pl.BlockSpec((1, 1) + block, lambda l, t: (1, l) + where_of(t))
    at_zero, at_one = grad_at
    return call(
        functools.partial(adam_kernel, rate, turned),
        (factor, master, moments, moments, *grads),
        [
            smem(), spec, first, second,
            pl.BlockSpec(grad_block, lambda l, t: (0, at_zero + t)),
            pl.BlockSpec(grad_block, lambda l, t: (0, at_one + t)),
        ],
        [(master.shape, f32)] * 3,
        out_specs=[spec] * 3,
        grid=(LAYERS, tiles),
        flops=20 * master.size,
    )


def swap(values, axis, bit):
    count = lax.axis_size(axis)
    return lax.ppermute(values, axis, [(i, i ^ bit) for i in range(count)])


def bit_orders(axis):
    count = lax.axis_size(axis).bit_length() - 1
    return list(range(count)), list(range(1, count)) + [0]


def swap_core(values, pieces=2):
    parts = jnp.split(values, pieces, axis=0)
    return jnp.concatenate([swap(part, "mp", 1) for part in parts], axis=0)


def gather_rows(values, axis, order):
    index = lax.axis_index(axis)
    share = values.shape
    for bit in order:
        other = swap(values, axis, 1 << bit)
        high = ((index >> bit) & 1) == 1
        values = jnp.stack([jnp.where(high, other, values), jnp.where(high, values, other)])
    done = list(reversed(order))
    count = len(order)
    turn = [done.index(bit) for bit in reversed(range(count))]
    values = values.transpose(turn + [count, count + 1])
    return values.reshape((-1,) + share[1:])


def gather_both(values, axis):
    first, second = bit_orders(axis)
    cut = (values.shape[1] // 2 + PAIR - 1) // PAIR * PAIR
    parts = [
        gather_rows(values[:, :cut], axis, first[::-1]),
        gather_rows(values[:, cut:], axis, second[::-1]),
    ]
    return jnp.concatenate(parts, axis=1)


class Scatter:

    def __init__(self, values, axis, cut=None):
        orders = bit_orders(axis)
        count = len(orders[0])
        self.axis, self.index, self.steps = axis, lax.axis_index(axis), count
        cut = values.shape[1] // 2 if cut is None else cut
        parts = (values[:, :cut], values[:, cut:])
        self.parts = [p.reshape((2,) * count + (-1, p.shape[1])) for p in parts]
        self.left = [list(order) for order in orders]

    def send(self):
        self.kept, self.came = [], []
        for values, left in zip(self.parts, self.left):
            bit = left[0]
            high = ((self.index >> bit) & 1) == 1
            at = sum(1 for other in left if other > bit)
            low_part = lax.index_in_dim(values, 0, at, keepdims=False)
            high_part = lax.index_in_dim(values, 1, at, keepdims=False)
            self.kept.append(jnp.where(high, high_part, low_part))
            self.came.append(swap(jnp.where(high, low_part, high_part), self.axis, 1 << bit))

    def wait_with(self, other):
        first, second, other = lax.optimization_barrier((self.came[0], self.came[1], other))
        self.came = [first, second]
        return other

    def add(self):
        self.left = [left[1:] for left in self.left]
        parts = [k.astype(f32) + c.astype(f32) for k, c in zip(self.kept, self.came)]
        self.parts = parts if not self.left[0] else [p.astype(bf16) for p in parts]

    def result(self):
        return jnp.concatenate(self.parts, axis=1)


def sum_all(values):
    for axis in ("mp", "dp"):
        bit = 1
        while bit < lax.axis_size(axis):
            values = values + swap(values, axis, bit)
            bit *= 2
    return values


def body(
    hidden_in,
    seg_lengths,
    partner,
    qkv_weight,
    out_weight,
    up_weight,
    down_weight,
    norm_params,
    emb_weight,
    log_scale,
    qkv_moments,
    out_moments,
    up_moments,
    down_moments,
    norm_moments,
    emb_moments,
    scale_moments,
):
    share = qkv_weight.shape[1]
    mp_count = lax.axis_size("mp")
    place = lax.axis_index("mp")
    core = place & 1
    far_chip = (place >> 1) == 1
    core_arr = core.reshape(1).astype(jnp.int32)

    def mine(first, second):
        return jnp.where(far_chip, second, first)

    def attn_pack(layer_at):
        return [qkv_weight[layer_at].reshape(share, 3 * WIDE), out_weight[layer_at].T]

    def mlp_pack(layer_at):
        return [up_weight[layer_at], down_weight[layer_at].T]

    norm_cols = jnp.pad(norm_params.reshape(4 * LAYERS, share).T, ((0, 0), (0, PAIR - 4 * LAYERS)))

    def packed(parts):
        return jnp.concatenate(parts, axis=1).astype(bf16)

    def gather(values):
        return lax.all_gather(values, "dp", axis=0, tiled=True)

    first_w = gather_both(packed(attn_pack(0) + [norm_cols]), "dp")
    middle_w = gather(packed(attn_pack(1) + mlp_pack(0)))
    last_w = gather(packed(mlp_pack(1) + [emb_weight]))
    attn_w = [first_w, middle_w]
    mlp_w = [(middle_w, 1), (last_w, 0)]
    nrm = first_w[:, 4 * WIDE : 4 * WIDE + 4 * LAYERS].T.astype(f32)
    w_emb = last_w[:, 2 * HID :]

    segment, offset = row_layout(seg_lengths[0])

    def own_order(values):
        blocks = values.reshape(2, 2, BLK)
        return jnp.where(core == 1, blocks[:, ::-1], blocks).reshape(ROW_LEN)

    segment = own_order(segment).astype(f32)
    offset = own_order(offset).astype(f32)
    seg_col = jnp.broadcast_to(segment[:, None], (ROW_LEN, PAIR))
    seg_row = jnp.broadcast_to(segment[None, :], (8, ROW_LEN))
    lane = jnp.arange(PAIR, dtype=jnp.int32)
    frequency = jnp.exp((lane % (HEAD_DIM // 2)).astype(f32) * (-2.0 * math.log(10000.0) / HEAD_DIM))
    angles = offset[:, None] * frequency[None, :]
    cosines = jnp.cos(angles)
    sines = jnp.where((lane % HEAD_DIM) < HEAD_DIM // 2, -1.0, 1.0)[None, :] * jnp.sin(angles)

    other_half = swap(hidden_in, "mp", 2)
    low = [mine(hidden_in, other_half), mine(other_half, hidden_in)]
    stream = [v.astype(f32) for v in low]

    def chip_sum(own, send):
        return (own.astype(f32) + swap_core(send).astype(f32)).astype(bf16)

    def cross(total, earlier=None):
        if earlier is not None:
            total, earlier = lax.optimization_barrier((total, earlier))
        return total, swap(total, "mp", 2), earlier

    kept = []
    sums = None
    for layer_at in range(LAYERS):
        streams, qkvs, norm_prev = [], [], []
        if layer_at > 0:
            stream, low = [], []
        for at in range(2):
            if layer_at > 0:
                h, hb, zz = norm_fwd(4 * layer_at - 2, normed[at], *sums[at], nrm)
                stream.append(h)
                low.append(hb)
                kept[-1][-1].append(zz)
            sib = swap(low[at], "mp", 1)
            streams += [low[at], sib]
            qkvs.append(qkv_project(low[at], sib, attn_w[layer_at], cosines, sines, at))
        o_a, lse_a, own, send = attend(
            0, core_arr, qkvs[0], qkvs[1], seg_col, seg_row, attn_w[layer_at], None
        )
        total_a, came_a, _ = cross(chip_sum(own, send))
        o_b, lse_b, own, send = attend(
            1, core_arr, qkvs[1], qkvs[0], seg_col, seg_row, attn_w[layer_at], total_a
        )
        total_b, came_b, came_a = cross(chip_sum(own, send), came_a)
        h_a, hb_a, z_a = norm_fwd(4 * layer_at, stream[0], total_a, came_a, nrm)
        sib_a = swap(hb_a, "mp", 1)
        zg_a, own, send = mlp(hb_a, sib_a, mlp_w[layer_at], None)
        next_a, next_came_a, came_b = cross(chip_sum(own, send), came_b)
        h_b, hb_b, z_b = norm_fwd(4 * layer_at, stream[1], total_b, came_b, nrm)
        sib_b = swap(hb_b, "mp", 1)
        zg_b, own, send = mlp(hb_b, sib_b, mlp_w[layer_at], None)
        next_b, next_came_b, next_came_a = cross(chip_sum(own, send), next_came_a)
        normed = [h_a, h_b]
        sums = [(next_a, next_came_a), (next_b, next_came_b)]
        kept.append(
            (streams, qkvs, [(o_a, lse_a), (o_b, lse_b)], [z_a, z_b], [hb_a, sib_a, hb_b, sib_b], [zg_a, zg_b], [])
        )
    stream, low = [], []
    for at in range(2):
        h, hb, zz = norm_fwd(4 * LAYERS - 2, normed[at], *sums[at], nrm)
        stream.append(h)
        low.append(hb)
        kept[-1][-1].append(zz)
    hidden_out = mine(stream[0], stream[1])

    emb_own = jnp.concatenate([dot_nn(low[0], w_emb), dot_nn(low[1], w_emb)], axis=0).astype(bf16)
    emb_all = jnp.concatenate([emb_own, swap(emb_own, "mp", 1)], axis=0)

    def loss_order(values):
        return values.reshape(2, 2, BLK).transpose(1, 0, 2).reshape(ROW_LEN)

    loss_seg = loss_order(segment)
    lengths = jnp.broadcast_to(
        jnp.pad(seg_lengths[0].astype(f32), (0, PAIR - SEGS), constant_values=1.0)[None], (8, PAIR)
    )
    partners = jnp.broadcast_to(
        jnp.pad(partner[0].astype(f32), (0, PAIR - SEGS), constant_values=-1.0)[None], (8, PAIR)
    )
    dx0, dx1, g_emb, loss_parts = loss_and_grads(
        log_scale,
        emb_all,
        jnp.broadcast_to(loss_seg[:, None], (ROW_LEN, PAIR)),
        jnp.broadcast_to(loss_seg[None, :], (8, ROW_LEN)),
        lengths,
        partners,
        low[0],
        low[1],
        w_emb,
    )

    grads = [dx0, dx1]
    pending = [(), ()]
    reduced = []
    norm_grads = [None] * LAYERS
    for layer_at in reversed(range(LAYERS)):
        streams, qkvs, attended, norm_a, hiddens, zgs, norm_b = kept[layer_at]
        row = 4 * layer_at + 2
        d_a, db_a, gain_a = norm_bwd(row, grads[0], pending[0], norm_b[0], nrm)
        sib_a = swap(db_a, "mp", 1)
        du_a, own, send = mlp_back(db_a, sib_a, zgs[0], mlp_w[layer_at], None)
        total_a = chip_sum(own, send)
        if pending[1]:
            total_a, came_a, came_b = cross(total_a, pending[1][1])
            if upper.left[0]:
                came_b = upper.wait_with(came_b)
                upper.add()
                upper.send()
            pending[1] = (pending[1][0], came_b)
        else:
            total_a, came_a, _ = cross(total_a)
        d_b, db_b, gain_b = norm_bwd(row, grads[1], pending[1], norm_b[1], nrm)
        sib_b = swap(db_b, "mp", 1)
        du_b, own, send = mlp_back(db_b, sib_b, zgs[1], mlp_w[layer_at], total_a)
        total_b, came_b, came_a = cross(chip_sum(own, send), came_a)
        if layer_at < LAYERS - 1:
            came_a = upper.wait_with(came_a)
            upper.add()
            upper.send()
        gains = [(gain_a + gain_b)[:2]]
        both = mlp_grads(hiddens, [db_a, sib_a, db_b, sib_b], [du_a, du_b], zgs, total_b)
        reduced.append(lax.psum_scatter(both, "dp", scatter_dimension=0, tiled=True))
        row = 4 * layer_at
        grad_a, low_a, gain_a = norm_bwd(row, d_a, (total_a, came_a), norm_a[0], nrm)
        sib_a = swap(low_a, "mp", 1)
        if layer_at < LAYERS - 1:
            came_b = upper.wait_with(came_b)
            upper.add()
            while upper.left[0]:
                upper.send()
                upper.add()
        grad_b, low_b, gain_b = norm_bwd(row, d_b, (total_b, came_b), norm_a[1], nrm)
        dattn = [low_a, sib_a, low_b, swap(low_b, "mp", 1)]
        dmixes = attend_back(
            core_arr, dattn, attn_w[layer_at], *qkvs, attended[0][0], attended[1][0],
            attended[0][1], attended[1][1], seg_col, seg_row, cosines, sines,
        )
        norm_grads[layer_at] = jnp.concatenate([(gain_a + gain_b)[:2]] + gains, axis=0)
        outs = [attended[0][0], attended[1][0]]
        grads = [grad_a, grad_b]
        if layer_at > 0:
            total_a, came_a, _ = cross(chip_sum(*qkv_back(dmixes[0], attn_w[layer_at], None)))
            total_b, came_b, came_a = cross(
                chip_sum(*qkv_back(dmixes[1], attn_w[layer_at], total_a)), came_a
            )
            pending = [(total_a, came_a), (total_b, came_b)]
            upper = Scatter(attn_grads(streams, dattn, dmixes, outs, total_a), "dp")
            upper.send()
        else:
            norm_rows = jnp.concatenate(norm_grads, axis=0)
            small = jnp.concatenate([g_emb, jnp.pad(norm_rows.T, ((0, 0), (0, PAIR - 4 * LAYERS)))], axis=1)
            last = attn_grads(streams, dattn, dmixes, outs, None, small.astype(bf16))
            lower = Scatter(last, "dp")
            fourth = upper.result()
            squares = jnp.sum(jnp.square(reduced[0].astype(f32))) + jnp.sum(jnp.square(fourth))
            while lower.left[0]:
                lower.send()
                if len(lower.left[0]) == lower.steps:
                    squares = lower.wait_with(squares)
                lower.add()
            third = lower.result()
            totals = []
            for at in range(2):
                own, send = qkv_back(dmixes[at], attn_w[layer_at], last)
                totals.append(own.astype(f32) + swap(send, "mp", 1).astype(f32))
            came = swap(mine(totals[1], totals[0]).astype(bf16), "mp", 2)
            hidden_grad = mine(grads[0], grads[1]) + (mine(totals[0], totals[1]) + came.astype(f32))

    first, second = reduced
    third, hidden_grad = lax.optimization_barrier((third, hidden_grad))
    small = third[:, 4 * WIDE :]
    small = small + swap(small, "mp", 1)
    emb_grad = small[:, :EMB]
    norm_grad = small[:, EMB : EMB + 4 * LAYERS].T.reshape(LAYERS, 2, 2, share)
    squares = (
        squares + jnp.sum(jnp.square(second.astype(f32))) + jnp.sum(jnp.square(third[:, : 4 * WIDE]))
        + jnp.sum(small * small) / mp_count
    )
    parts = jnp.concatenate([loss_parts[:2], jnp.zeros((6, PAIR), f32)], axis=0)
    loss_here = jnp.sum(parts[0]) / mp_count
    dscale_here = jnp.sum(parts[1]) / mp_count
    vector = jnp.where(lane == 0, squares, jnp.where(lane == 1, dscale_here, jnp.where(lane == 2, loss_here, 0.0)))
    vector = sum_all(jnp.broadcast_to(vector[None], (8, PAIR)))
    total_squares = vector[0, 0]
    scale_grad = vector[0, 1:2]
    loss_total = vector[0, 2]
    norm_value = jnp.sqrt(total_squares + scale_grad[0] * scale_grad[0] + 1e-06)
    factor = clip_limit / jnp.maximum(norm_value, clip_limit)
    step_f = jnp.asarray(STEP, f32)
    factor_arr = factor.reshape(1)
    qkv_step = adam_step(
        factor_arr, qkv_weight.transpose(0, 2, 1, 3), qkv_moments.transpose(0, 1, 3, 2, 4), (third, fourth),
        3, (1, share, WIDE), lambda t: (t, 0, 0), (share, WIDE), (0, 0), D ** (-0.5),
    )
    qkv_new, qkv_first, qkv_second = [v.transpose(0, 2, 1, 3) for v in qkv_step]
    out_new, out_first, out_second = adam_step(
        factor_arr, out_weight, out_moments, (third, fourth),
        1, (WIDE, share), lambda t: (t, 0), (share, WIDE), (3, 3), (D * SEGS // ROW_LEN) ** (-0.5), True,
    )
    up_new, up_first, up_second = adam_step(
        factor_arr, up_weight, up_moments, (second, first),
        2, (share, HALF), lambda t: (0, t), (share, HALF), (0, 0), D ** (-0.5),
    )
    down_new, down_first, down_second = adam_step(
        factor_arr, down_weight, down_moments, (second, first),
        4, (TILE, share), lambda t: (t, 0), (share, TILE), (4, 4), FF ** (-0.5), True,
    )
    norm_new, norm_first, norm_second = adamw_update(norm_params, norm_moments, norm_grad, factor, 0.5, step_f)
    emb_new, emb_first, emb_second = adamw_update(emb_weight, emb_moments, emb_grad, factor, D ** (-0.5), step_f)
    scale_new, scale_first, scale_second = adamw_update(log_scale, scale_moments, scale_grad, factor, 1.0, step_f)
    return (
        hidden_out,
        hidden_grad,
        loss_total.reshape(1),
        norm_value.reshape(1),
        qkv_new,
        qkv_first,
        qkv_second,
        out_new,
        out_first,
        out_second,
        up_new,
        up_first,
        up_second,
        down_new,
        down_first,
        down_second,
        norm_new,
        norm_first,
        norm_second,
        emb_new,
        emb_first,
        emb_second,
        scale_new,
        scale_first,
        scale_second,
    )


def solution(mesh):
    placed = (
        P(("dp", "mp"), None),
        P("dp", None),
        P("dp", None),
        P(None, "dp", None, "mp"),
        P(None, "mp", "dp"),
        P(None, "dp", "mp"),
        P(None, "mp", "dp"),
        P(None, None, None, "dp"),
        P("dp", None),
        P(),
        P(None, None, "dp", None, "mp"),
        P(None, None, "mp", "dp"),
        P(None, None, "dp", "mp"),
        P(None, None, "mp", "dp"),
        P(None, None, None, None, "dp"),
        P(None, "dp", None),
        P(),
    )
    results = (P(("dp", "mp"), None), P(("dp", "mp"), None), P(), P())
    for at in (3, 4, 5, 6, 7, 8, 9):
        results += (placed[at],) * 3
    return jax.shard_map(body, mesh=mesh, in_specs=placed, out_specs=results, check_vma=False)
```

```python
import functools
import math

import jax
import jax.numpy as jnp
from jax import lax
from jax.experimental import pallas as pl
from jax.experimental.pallas import tpu as pltpu
from jax.sharding import PartitionSpec as P

D = 1024
HEAD_DIM = 64
FF = 4096
EMB = 128
LAYERS = 2
STEP = 5
ROW_LEN = 1024
SEGS = 8

BLK = 256
HALF = 512
WIDE = 256
HID = 1024
PAIR = 128
PAIRS = WIDE // PAIR
MIB = 1 << 20
COST = 1

f32 = jnp.float32
bf16 = jnp.bfloat16
best = lax.Precision.HIGHEST
sharpness = 0.05
clip_limit = 1.0

OUT_AT = 3 * WIDE


def dot_nn(left, right):
    return lax.dot_general(left, right, (((1,), (0,)), ((), ())), preferred_element_type=f32)


def dot_nt(left, right):
    return lax.dot_general(left, right, (((1,), (1,)), ((), ())), preferred_element_type=f32)


def dot_tn(left, right):
    return lax.dot_general(left, right, (((0,), (0,)), ((), ())), preferred_element_type=f32)


def whole(shape):
    return pl.BlockSpec(shape, lambda *_: (0,) * len(shape))


def call(kernel, args, in_specs, outs, out_specs=None, grid=(1,), scratch=(), flops=0, vmem=32, alias=None,
         keep=(), after=None, far=()):
    out_shape = [
        pltpu.HBM(s, d) if i in keep else jax.ShapeDtypeStruct(s, d) for i, (s, d) in enumerate(outs)
    ]
    if out_specs is None:
        out_specs = [whole(s) for s, _ in outs]
    args = [pltpu.with_memory_space_constraint(a, pltpu.HBM) if i in far else a for i, a in enumerate(args)]
    in_specs = list(in_specs)
    moved = sum(math.prod(a.shape) * a.dtype.itemsize for a in args if a.size < 3 * MIB)
    moved += sum(math.prod(s) * jnp.dtype(d).itemsize for s, d in outs)
    body_fn = kernel
    if after is not None:
        count = len(args)
        args = args + [after]
        in_specs = in_specs + [pl.BlockSpec(memory_space=pl.ANY)]

        def body_fn(*refs):
            kernel(*refs[:count], *refs[count + 1 :])

    return pl.pallas_call(
        body_fn,
        grid=grid,
        in_specs=in_specs,
        out_specs=out_specs,
        out_shape=out_shape,
        scratch_shapes=list(scratch),
        input_output_aliases=alias or {},
        compiler_params=pltpu.CompilerParams(
            dimension_semantics=("arbitrary",) * len(grid), vmem_limit_bytes=vmem * MIB
        ),
        cost_estimate=pl.CostEstimate(flops=int(flops * COST), bytes_accessed=int(moved * COST), transcendentals=0),
    )(*args)


def smem():
    return pl.BlockSpec(memory_space=pltpu.SMEM)


def halves(values):
    high = values.astype(bf16)
    return high, (values - high.astype(f32)).astype(bf16)


def norm_fwd_kernel(row, with_sums, *refs):
    if with_sums:
        x_ref, s_ref, r_ref, n_ref, h_ref, hb_ref, z_ref = refs
        v = x_ref[...].astype(f32) + (s_ref[...].astype(f32) + r_ref[...].astype(f32))
    else:
        x_ref, n_ref, h_ref, hb_ref, z_ref = refs
        v = x_ref[...].astype(f32)
    cen = v - jnp.mean(v, axis=1, keepdims=True)
    var = jnp.mean(cen * cen, axis=1, keepdims=True)
    rstd = lax.rsqrt(var + 1e-05)
    z = cen * rstd
    h = z * n_ref[row : row + 1, :] + n_ref[row + 1 : row + 2, :]
    h_ref[...] = h
    hb_ref[...] = h.astype(bf16)
    z_ref[:, 0:D] = z.astype(bf16)
    high, rest = halves(rstd)
    lane = lax.broadcasted_iota(jnp.int32, (BLK, PAIR), 1)
    z_ref[:, D:] = jnp.where(lane < 1, high.astype(f32), rest.astype(f32)).astype(bf16)


def norm_fwd(row, x, s, r, nrm):
    blk = whole((BLK, D))
    return call(
        functools.partial(norm_fwd_kernel, row, True),
        (x, s, r, nrm),
        [blk, blk, blk, whole(nrm.shape)],
        [((BLK, D), f32), ((BLK, D), bf16), ((BLK, D + PAIR), bf16)],
        flops=BLK * D * 10,
        keep=(2,),
    )


def norm_bwd_kernel(row, with_sums, *refs):
    if with_sums:
        d_ref, s_ref, r_ref, z_ref, n_ref, o_ref, ob_ref, g_ref = refs
        dy = d_ref[...] + (s_ref[...].astype(f32) + r_ref[...].astype(f32))
    else:
        d_ref, z_ref, n_ref, o_ref, ob_ref, g_ref = refs
        dy = d_ref[...]
    z = z_ref[:, 0:D].astype(f32)
    rstd = z_ref[:, D : D + 1].astype(f32) + z_ref[:, D + 1 : D + 2].astype(f32)
    dz = dy * n_ref[row : row + 1, :]
    m1 = jnp.mean(dz, axis=1, keepdims=True)
    m2 = jnp.mean(dz * z, axis=1, keepdims=True)
    dr = (dz - m1 - z * m2) * rstd
    o_ref[...] = dr
    ob_ref[...] = dr.astype(bf16)
    g_ref[...] = jnp.concatenate(
        [jnp.sum(dy * z, axis=0, keepdims=True), jnp.sum(dy, axis=0, keepdims=True), jnp.zeros((6, D), f32)],
        axis=0,
    )


def norm_bwd(row, d, sums, z, nrm):
    blk = whole((BLK, D))
    args = (d,) + tuple(sums) + (z, nrm)
    return call(
        functools.partial(norm_bwd_kernel, row, len(sums) > 0),
        args,
        [blk] * (1 + len(sums)) + [whole((BLK, D + PAIR)), whole(nrm.shape)],
        [((BLK, D), f32), ((BLK, D), bf16), ((8, D), f32)],
        flops=BLK * D * 14,
        far=(1 + len(sums),),
    )


def rope_lanes(values, cosines, sines):
    lane = lax.broadcasted_iota(jnp.int32, values.shape, 1)
    low = (lane & (HEAD_DIM - 1)) < HEAD_DIM // 2
    swapped = jnp.where(
        low, pltpu.roll(values, PAIR - HEAD_DIM // 2, 1), pltpu.roll(values, HEAD_DIM // 2, 1)
    )
    return values * cosines + swapped * sines


def qkv_kernel(xo_ref, xs_ref, w_ref, c_ref, s_ref, m_ref):
    for at, x_ref in enumerate((xo_ref, xs_ref)):
        rows = slice(at * BLK, (at + 1) * BLK)
        mix = dot_nn(x_ref[...], w_ref[...])
        cosines, sines = c_ref[rows, :], s_ref[rows, :]
        for p in range(PAIRS):
            lanes = slice(p * PAIR, (p + 1) * PAIR)
            q = rope_lanes(mix[:, p * PAIR : (p + 1) * PAIR], cosines, sines).astype(bf16)
            m_ref[rows, lanes] = q * HEAD_DIM ** (-0.5)
            lanes = slice(WIDE + p * PAIR, WIDE + (p + 1) * PAIR)
            m_ref[rows, lanes] = rope_lanes(mix[:, lanes], cosines, sines).astype(bf16)
        m_ref[rows, 2 * WIDE :] = mix[:, 2 * WIDE :].astype(bf16)


def qkv_project(x_own, x_sib, weights, cosines, sines, at):
    blk = whole((BLK, D))
    tab = pl.BlockSpec((HALF, PAIR), lambda *_: (at, 0))
    return call(
        qkv_kernel,
        (x_own, x_sib, weights, cosines, sines),
        [blk, blk, pl.BlockSpec((D, 3 * WIDE), lambda *_: (0, 0)), tab, tab],
        [((HALF, 3 * WIDE), bf16)],
        flops=2 * HALF * D * 3 * WIDE,
        keep=(0,),
    )[0]


def near_places(core, at):
    if at == 0:
        return 1 - core, core
    return core, 1 - core


def attend_kernel(at, core_ref, m_ref, mo_ref, sc_ref, sco_ref, sr_ref, w_ref, o_ref, l_ref, own_ref, send_ref):
    q_ref, k_ref, v_ref = [m_ref.at[:, i * WIDE : (i + 1) * WIDE] for i in range(3)]
    ko_ref, vo_ref = [mo_ref.at[:, i * WIDE : (i + 1) * WIDE] for i in (1, 2)]
    near, cross = near_places(core_ref[0], at)
    cross_rows = pl.ds(pl.multiple_of(cross * BLK, BLK), BLK)
    row_at = lax.broadcasted_iota(jnp.int32, (PAIR, BLK), 0)
    lane_at = lax.broadcasted_iota(jnp.int32, (BLK, PAIR), 1)
    seg_main = sc_ref[...]
    seg_main = jnp.concatenate([seg_main, seg_main], axis=1)
    seg_cross = sco_ref[cross_rows, :]
    seg_cross = jnp.concatenate([seg_cross, seg_cross], axis=1)
    l_ref[...] = jnp.zeros(l_ref.shape, f32)
    for is_near in (False, True):
        place = near if is_near else 1 - near
        start = pl.multiple_of(place * BLK, BLK)
        rows = pl.ds(start, BLK)
        seg_q = sr_ref[0:1, rows]
        bias = jnp.where(seg_main == seg_q, 0.0, -1e30)
        if is_near:
            bias_cross = jnp.where(seg_cross == seg_q, 0.0, -1e30)
        for p in range(PAIRS):
            lanes = slice(p * PAIR, (p + 1) * PAIR)
            keys = k_ref[:, lanes]
            values_t = v_ref[:, lanes].T
            queries = q_ref[rows, lanes]
            if is_near:
                keys_cross = ko_ref[cross_rows, lanes]
                values_cross_t = vo_ref[cross_rows, lanes].T
            parts = []
            for h in range(2):
                q = jnp.where((lane_at >= HEAD_DIM) == (h == 1), queries, jnp.zeros_like(queries))
                scores = dot_nt(keys, q) + bias
                top = jnp.max(scores, axis=0, keepdims=True)
                if is_near:
                    scores_cross = dot_nt(keys_cross, q) + bias_cross
                    top = jnp.maximum(top, jnp.max(scores_cross, axis=0, keepdims=True))
                e = jnp.exp(scores - top)
                total = jnp.sum(e, axis=0, keepdims=True)
                mixed = dot_nn(values_t, e.astype(bf16))
                if is_near:
                    e = jnp.exp(scores_cross - top)
                    total = total + jnp.sum(e, axis=0, keepdims=True)
                    mixed = mixed + dot_nn(values_cross_t, e.astype(bf16))
                parts.append(mixed / total)
                head = 2 * p + h
                l_ref[head : head + 1, rows] = top + jnp.log(total)
            both = jnp.where(row_at < HEAD_DIM, parts[0], parts[1])
            o_ref[rows, lanes] = both.T.astype(bf16)
    own_ref[...] = dot_nt(o_ref[0:BLK, :], w_ref[...]).astype(bf16)
    send_ref[...] = dot_nt(o_ref[BLK:HALF, :], w_ref[...]).astype(bf16)


def attend(at, core, qkv, qkv_other, seg_col, seg_row, weights, after):
    mix = whole((HALF, 3 * WIDE))
    return call(
        functools.partial(attend_kernel, at),
        (core, qkv, qkv_other, seg_col, seg_col, seg_row, weights),
        [
            smem(), mix, mix,
            pl.BlockSpec((HALF, PAIR), lambda *_: (at, 0)),
            pl.BlockSpec((HALF, PAIR), lambda *_: (1 - at, 0)),
            pl.BlockSpec((8, HALF), lambda *_: (0, at)),
            pl.BlockSpec((D, WIDE), lambda *_: (0, OUT_AT // WIDE)),
        ],
        [((HALF, WIDE), bf16), ((8, HALF), f32), ((BLK, D), bf16), ((BLK, D), bf16)],
        flops=4 * 4 * 5 * BLK * BLK * PAIR + 2 * HALF * WIDE * D,
        far=(1, 2),
        keep=(0, 1),
        after=after,
    )


def attend_back_kernel(core_ref, d0o, d0s, d1o, d1s, w_ref, mix0, mix1, o0, o1, l0, l1,
                       sc_ref, sr_ref, c_ref, s_ref, m0_ref, m1_ref,
                       dout_ref, dk_ref, dv_ref, dq_ref):
    for i, d in enumerate((d0o, d0s, d1o, d1s)):
        dout_ref[i // 2, (i % 2) * BLK : (i % 2 + 1) * BLK, :] = dot_nn(d[...], w_ref[...]).astype(bf16)
    dk_ref[...] = jnp.zeros(dk_ref.shape, f32)
    dv_ref[...] = jnp.zeros(dv_ref.shape, f32)
    row_at = lax.broadcasted_iota(jnp.int32, (PAIR, 1), 0)
    lane_at = lax.broadcasted_iota(jnp.int32, (1, PAIR), 1)
    scaling = HEAD_DIM ** (-0.5)
    q_refs, k_refs, v_refs = [
        [m.at[:, i * WIDE : (i + 1) * WIDE] for m in (mix0, mix1)] for i in range(3)
    ]
    o_refs, l_refs = (o0, o1), (l0, l1)
    for at in range(2):
        near, cross = near_places(core_ref[0], at)
        cross_rows = pl.ds(pl.multiple_of(cross * BLK, BLK), BLK)
        cross_full = pl.ds(pl.multiple_of((1 - at) * HALF + cross * BLK, BLK), BLK)
        seg_main = sc_ref[at * HALF : (at + 1) * HALF, :]
        seg_main = jnp.concatenate([seg_main, seg_main], axis=1)
        seg_cross = sc_ref[cross_full, :]
        seg_cross = jnp.concatenate([seg_cross, seg_cross], axis=1)
        for is_near in (False, True):
            place = near if is_near else 1 - near
            rows = pl.ds(pl.multiple_of(place * BLK, BLK), BLK)
            seg_q = sr_ref[0:1, pl.ds(pl.multiple_of(at * HALF + place * BLK, BLK), BLK)]
            bias = jnp.where(seg_main == seg_q, 0.0, -1e30)
            if is_near:
                bias_cross = jnp.where(seg_cross == seg_q, 0.0, -1e30)
            for p in range(PAIRS):
                lanes = slice(p * PAIR, (p + 1) * PAIR)
                keys, values = k_refs[at][:, lanes], v_refs[at][:, lanes]
                keys_t = keys.T
                queries, douts = q_refs[at][rows, lanes], dout_ref[at, rows, lanes]
                if is_near:
                    keys_cross = k_refs[1 - at][cross_rows, lanes]
                    values_cross = v_refs[1 - at][cross_rows, lanes]
                    keys_cross_t = keys_cross.T
                products = (douts.astype(f32) * o_refs[at][rows, lanes].astype(f32)).T
                dq_t = jnp.zeros((PAIR, BLK), f32)
                for h in range(2):
                    in_lanes = (lane_at >= HEAD_DIM) == (h == 1)
                    in_rows = (row_at >= HEAD_DIM) == (h == 1)
                    q = jnp.where(in_lanes, queries, jnp.zeros_like(queries))
                    d = jnp.where(in_lanes, douts, jnp.zeros_like(douts))
                    delta = jnp.sum(products[h * HEAD_DIM : (h + 1) * HEAD_DIM, :], axis=0, keepdims=True)
                    lse = l_refs[at][2 * p + h : 2 * p + h + 1, rows]
                    kt = jnp.where(in_rows, keys_t, jnp.zeros_like(keys_t))
                    probs = jnp.exp(dot_nt(keys, q) + bias - lse)
                    dscores = (probs * (dot_nt(values, d) - delta)).astype(bf16)
                    dv_ref[at, :, lanes] += dot_nn(probs.astype(bf16), d)
                    dk_ref[at, :, lanes] += dot_nn(dscores, q)
                    dq_t = dq_t + dot_nn(kt, dscores)
                    if is_near:
                        kt = jnp.where(in_rows, keys_cross_t, jnp.zeros_like(keys_cross_t))
                        probs = jnp.exp(dot_nt(keys_cross, q) + bias_cross - lse)
                        dscores = (probs * (dot_nt(values_cross, d) - delta)).astype(bf16)
                        dv_ref[1 - at, cross_rows, lanes] += dot_nn(probs.astype(bf16), d)
                        dk_ref[1 - at, cross_rows, lanes] += dot_nn(dscores, q)
                        dq_t = dq_t + dot_nn(kt, dscores)
                dq_ref[at, rows, lanes] = dq_t.T * scaling
    for at, m_ref in enumerate((m0_ref, m1_ref)):
        rows = slice(at * HALF, (at + 1) * HALF)
        cosines, sines = c_ref[rows, :], -s_ref[rows, :]
        for p in range(PAIRS):
            lanes = slice(p * PAIR, (p + 1) * PAIR)
            m_ref[:, p * PAIR : (p + 1) * PAIR] = rope_lanes(dq_ref[at, :, lanes], cosines, sines).astype(bf16)
            m_ref[:, WIDE + p * PAIR : WIDE + (p + 1) * PAIR] = rope_lanes(
                dk_ref[at, :, lanes], cosines, sines
            ).astype(bf16)
        m_ref[:, 2 * WIDE :] = dv_ref[at].astype(bf16)


def attend_back(core, dblocks, weights, qkv_a, qkv_b, o_a, o_b, l_a, l_b, seg_col, seg_row, cosines, sines):
    blk, half, low, mix = whole((BLK, D)), whole((HALF, WIDE)), whole((8, HALF)), whole((HALF, 3 * WIDE))
    tab = whole((ROW_LEN, PAIR))
    return call(
        attend_back_kernel,
        (core, *dblocks, weights, qkv_a, qkv_b, o_a, o_b, l_a, l_b, seg_col, seg_row, cosines, sines),
        [smem(), blk, blk, blk, blk, pl.BlockSpec((D, WIDE), lambda *_: (0, OUT_AT // WIDE))]
        + [mix, mix, half, half]
        + [low, low, tab, whole((8, ROW_LEN)), tab, tab],
        [((HALF, 3 * WIDE), bf16)] * 2,
        scratch=[
            pltpu.VMEM((2, HALF, WIDE), bf16),
            pltpu.VMEM((2, HALF, WIDE), f32),
            pltpu.VMEM((2, HALF, WIDE), f32),
            pltpu.VMEM((2, HALF, WIDE), f32),
        ],
        flops=10 * 4 * 10 * BLK * BLK * PAIR + 2 * ROW_LEN * WIDE * D,
        far=(6, 7, 8, 9, 10, 11),
    )


def spread_kernel(m_ref, w_ref, own_ref, send_ref):
    own_ref[...] = dot_nt(m_ref[0:BLK, :], w_ref[...]).astype(bf16)
    send_ref[...] = dot_nt(m_ref[BLK:HALF, :], w_ref[...]).astype(bf16)


def qkv_back(dmix, weights, after):
    return call(
        spread_kernel,
        (dmix, weights),
        [whole(dmix.shape), pl.BlockSpec((D, 3 * WIDE), lambda *_: (0, 0))],
        [((BLK, D), bf16)] * 2,
        flops=2 * HALF * D * 3 * WIDE,
        after=after,
    )


TILE = 256
TILES = HID // TILE


def gelu_pair(u):
    half = jnp.exp(u * u * -0.5)
    t = 1.0 / (1.0 + (0.3275911 * 0.5 ** 0.5) * jnp.abs(u))
    poly = t * (
        0.5 * 0.254829592
        + t * (0.5 * -0.284496736 + t * (0.5 * 1.421413741 + t * (0.5 * -1.453152027 + t * (0.5 * 1.061405429))))
    )
    tail = poly * half
    phi = jnp.where(u >= 0.0, 1.0 - tail, tail)
    return u * phi, phi + u * half * (1.0 / math.sqrt(2.0 * math.pi))


def mlp_kernel(ho_ref, hs_ref, up_ref, down_ref, zg_ref, own_ref, send_ref):
    for at, (h_ref, p_ref) in enumerate(((ho_ref, own_ref), (hs_ref, send_ref))):
        rows = slice(at * BLK, (at + 1) * BLK)
        value, slope = gelu_pair(dot_nn(h_ref[...], up_ref[...]))
        z = value.astype(bf16)
        zg_ref[rows, 0:HID] = z
        zg_ref[rows, HID:] = slope.astype(bf16)
        p_ref[...] = dot_nt(z, down_ref[...]).astype(bf16)


def mlp(h_own, h_sib, weights, after):
    blk = whole((BLK, D))
    array, first = weights
    return call(
        mlp_kernel,
        (h_own, h_sib, array, array),
        [
            blk, blk,
            pl.BlockSpec((D, HID), lambda *_: (0, first)),
            pl.BlockSpec((D, HID), lambda *_: (0, first + 1)),
        ],
        [((HALF, 2 * HID), bf16), ((BLK, D), bf16), ((BLK, D), bf16)],
        flops=4 * HALF * D * HID,
        keep=(0,),
        after=after,
    )


def mlp_back_kernel(do_ref, ds_ref, g_ref, up_ref, down_ref, du_ref, own_ref, send_ref):
    for at, (d_ref, p_ref) in enumerate(((do_ref, own_ref), (ds_ref, send_ref))):
        rows = slice(at * BLK, (at + 1) * BLK)
        du = (dot_nn(d_ref[...], down_ref[...]) * g_ref[rows, :].astype(f32)).astype(bf16)
        du_ref[rows, :] = du
        p_ref[...] = dot_nt(du, up_ref[...]).astype(bf16)


def mlp_back(d_own, d_sib, zg, weights, after):
    blk = whole((BLK, D))
    array, first = weights
    return call(
        mlp_back_kernel,
        (d_own, d_sib, zg, array, array),
        [
            blk, blk,
            pl.BlockSpec((HALF, HID), lambda *_: (0, 1)),
            pl.BlockSpec((D, HID), lambda *_: (0, first)),
            pl.BlockSpec((D, HID), lambda *_: (0, first + 1)),
        ],
        [((HALF, HID), bf16), ((BLK, D), bf16), ((BLK, D), bf16)],
        flops=4 * HALF * D * HID,
        far=(2,),
        after=after,
    )


def turn_into(t_ref, x_refs):
    for i, x in enumerate(x_refs):
        t_ref[:, i * BLK : (i + 1) * BLK] = x[...].T


def grad_tile(t_ref, y_refs):
    first, second = y_refs
    return (dot_nn(t_ref[:, 0:HALF], first[...]) + dot_nn(t_ref[:, HALF:], second[...])).astype(bf16)


def mlp_grad_kernel(x0, x1, x2, x3, d0, d1, d2, d3, u0, u1, z0, z1, g_ref, t_ref):
    step = pl.program_id(0)

    @pl.when(step == 0)
    def _():
        turn_into(t_ref, (x0, x1, x2, x3))

    @pl.when(step == HID // HALF)
    def _():
        turn_into(t_ref, (d0, d1, d2, d3))

    @pl.when(step < HID // HALF)
    def _():
        g_ref[...] = grad_tile(t_ref, (u0, u1))

    @pl.when(step >= HID // HALF)
    def _():
        g_ref[...] = grad_tile(t_ref, (z0, z1))


def mlp_grads(hidden, dblocks, dus, zs, after):
    blk = whole((BLK, D))
    tiles = HID // HALF
    first = pl.BlockSpec((HALF, HALF), lambda t: (0, jnp.minimum(t, tiles - 1)))
    second = pl.BlockSpec((HALF, HALF), lambda t: (0, jnp.maximum(t - tiles, 0)))
    return call(
        mlp_grad_kernel,
        (*hidden, *dblocks, *dus, *zs),
        [blk] * 8 + [first] * 2 + [second] * 2,
        [((D, 2 * HID), bf16)],
        out_specs=[pl.BlockSpec((D, HALF), lambda t: (0, t))],
        grid=(2 * tiles,),
        scratch=[pltpu.VMEM((D, ROW_LEN), bf16)],
        flops=4 * ROW_LEN * D * HID,
        keep=(0,),
        after=after,
    )[0]


def attn_grad_kernel(with_small, x0, x1, x2, x3, d0, d1, d2, d3, m0, m1, o0, o1, *refs):
    g_ref, t_ref = refs[-2:]
    step = pl.program_id(0)

    @pl.when(step == 0)
    def _():
        turn_into(t_ref, (x0, x1, x2, x3))

    @pl.when(step == 3)
    def _():
        turn_into(t_ref, (d0, d1, d2, d3))

    @pl.when(step < 3)
    def _():
        g_ref[...] = grad_tile(t_ref, (m0, m1))

    @pl.when(step == 3)
    def _():
        g_ref[...] = grad_tile(t_ref, (o0, o1))

    if with_small:

        @pl.when(step == 4)
        def _():
            g_ref[...] = refs[0][...]


def attn_grads(streams, dblocks, dmixes, outs, after, small=None):
    blk = whole((BLK, D))
    first = pl.BlockSpec((HALF, WIDE), lambda t: (0, jnp.minimum(t, 2)))
    args = (*streams, *dblocks, *dmixes, *outs) + (() if small is None else (small,))
    specs = [blk] * 8 + [first] * 2 + [whole((HALF, WIDE))] * 2
    specs += [] if small is None else [whole((D, WIDE))]
    steps = 4 if small is None else 5
    return call(
        functools.partial(attn_grad_kernel, small is not None),
        args,
        specs,
        [((D, steps * WIDE), bf16)],
        out_specs=[pl.BlockSpec((D, WIDE), lambda t: (0, t))],
        grid=(steps,),
        scratch=[pltpu.VMEM((D, ROW_LEN), bf16)],
        flops=2 * ROW_LEN * D * 4 * WIDE,
        after=after,
    )[0]


def loss_kernel(ls_ref, e_ref, seg_ref, segr_ref, len_ref, par_ref, x0_ref, x1_ref, we_ref,
                dx0_ref, dx1_ref, ge_ref, out_ref, sim_ref, b_ref, ll_ref, de_ref):
    tokens = ROW_LEN
    mine = HALF
    width_blk = BLK
    emb = e_ref[...].astype(f32)
    emb_t = emb.T
    lanes = lax.broadcasted_iota(jnp.int32, (tokens, PAIR), 1)
    label_col = lanes.astype(f32)
    member = (seg_ref[...] == label_col).astype(bf16)
    rows16 = lax.broadcasted_iota(jnp.int32, (16, tokens), 0).astype(f32)
    member_t = (jnp.broadcast_to(segr_ref[0:1, :], (16, tokens)) == rows16).astype(bf16)
    scale = jnp.exp(ls_ref[0])
    cls = lax.broadcasted_iota(jnp.int32, (16, PAIR), 0)
    seg = lax.broadcasted_iota(jnp.int32, (16, PAIR), 1)
    real = (cls < SEGS) & (seg < SEGS)
    allowed = (cls != seg) & real
    lengths = len_ref[0:1, :]
    chosen = (cls.astype(f32) == par_ref[0:1, :]) & real
    loss = jnp.zeros((1, PAIR), f32)
    dscale = jnp.zeros((1, PAIR), f32)
    de_ref[...] = jnp.zeros(de_ref.shape, f32)
    for width in (EMB, EMB * 3 // 4, EMB // 2):
        kept = jnp.where(lanes < width, emb, 0.0)
        r_col = lax.rsqrt(jnp.sum(kept * kept, axis=1, keepdims=True) + 1e-06)
        kept_low = kept.astype(bf16)
        row_of = lax.broadcasted_iota(jnp.int32, (PAIR, tokens), 0)
        kept_t = jnp.where(row_of < width, emb_t, 0.0)
        r_row = lax.rsqrt(jnp.sum(kept_t * kept_t, axis=0, keepdims=True) + 1e-06)
        b_ref[16:24, :] = jnp.broadcast_to(r_row, (8, tokens))

        def sims(i, carry):
            at = pl.multiple_of(i * width_blk, width_blk)
            cols = pl.ds(at, width_blk)
            other = jnp.where(lanes[0:width_blk, :] < width, e_ref[cols, :], jnp.zeros((width_blk, PAIR), bf16))
            near = dot_nt(kept_low, other)
            expo = jnp.exp(near * r_col * (b_ref[16:17, cols] * (1.0 / sharpness)) - 1.0 / sharpness)
            sim_ref[:, cols] = expo
            ll_ref[:, cols] = dot_nn(member_t, expo.astype(bf16))
            return carry

        lax.fori_loop(0, tokens // width_blk, sims, 0)
        totals = ll_ref[...]
        sum_rows = lax.broadcasted_iota(jnp.int32, totals.shape, 0)
        totals = jnp.where(sum_rows < SEGS, totals, 1.0)
        soft = sharpness * jnp.log(totals) + 1.0
        score = jnp.dot(soft, member.astype(f32), precision=best, preferred_element_type=f32) / lengths
        logits = jnp.where(allowed, scale * score, -1e30)
        top = jnp.max(logits, axis=0, keepdims=True)
        powers = jnp.exp(logits - top)
        summed = jnp.sum(powers, axis=0, keepdims=True)
        picked = jnp.sum(jnp.where(chosen, logits, 0.0), axis=0, keepdims=True)
        live = seg[0:1, :] < SEGS
        loss = loss + jnp.where(live, top + jnp.log(summed) - picked, 0.0)
        dlogit = jnp.where(allowed, powers / summed - chosen.astype(f32), 0.0)
        dscale = dscale + jnp.sum(dlogit * jnp.where(allowed, logits, 0.0), axis=0, keepdims=True)
        dscore = dlogit * scale / lengths
        dsoft = jnp.dot(dscore, jnp.concatenate([member_t.astype(f32), jnp.zeros((PAIR - 16, tokens), f32)], axis=0),
                        precision=best, preferred_element_type=f32)
        coef = dsoft / totals
        b_ref[0:16, :] = coef
        coef_high, coef_rest = halves(coef)
        left = jnp.concatenate([member_t, member_t, coef_high, coef_rest], axis=0)
        keep_t = kept_t.astype(bf16)

        def pulls(i, carry):
            at = pl.multiple_of(i * width_blk, width_blk)
            cols = pl.ds(at, width_blk)
            here_high, here_rest = halves(b_ref[0:16, cols])
            member_here = (
                jnp.broadcast_to(segr_ref[0:1, cols], (16, width_blk)) == rows16[:, 0:width_blk]
            ).astype(bf16)
            right = jnp.concatenate([here_high, here_rest, member_here, member_here], axis=0)
            pull = dot_tn(left, right) * sim_ref[:, cols] * r_col
            high, rest = halves(pull)
            de = dot_nn(keep_t, high) + dot_nn(keep_t, rest)
            r_here = b_ref[16:17, cols]
            e_here = jnp.where(lanes[0:width_blk, :] < width, e_ref[cols, :].astype(f32), 0.0).T
            along = jnp.sum(e_here * de, axis=0, keepdims=True)
            de_ref[:, cols] += r_here * de - (r_here * r_here * r_here * along) * e_here
            return carry

        lax.fori_loop(0, mine // width_blk, pulls, 0)
    de = de_ref[...].T.astype(bf16)
    dx0_ref[...] = dot_nt(de[0:BLK, :], we_ref[...])
    dx1_ref[...] = dot_nt(de[BLK:HALF, :], we_ref[...])
    ge_ref[...] = dot_tn(x0_ref[...], de[0:BLK, :]) + dot_tn(x1_ref[...], de[BLK:HALF, :])
    out_ref[...] = jnp.concatenate([loss, dscale, jnp.zeros((6, PAIR), f32)], axis=0)


def loss_and_grads(log_scale, emb, seg_col, seg_row, lengths, partner, x0, x1, w_emb):
    blk = whole((BLK, D))
    return call(
        loss_kernel,
        (log_scale, emb, seg_col, seg_row, lengths, partner, x0, x1, w_emb),
        [
            smem(), whole((ROW_LEN, EMB)), whole((ROW_LEN, PAIR)), whole((8, ROW_LEN)),
            whole((8, PAIR)), whole((8, PAIR)), blk, blk, whole((D, EMB)),
        ],
        [((BLK, D), f32), ((BLK, D), f32), ((D, EMB), f32), ((8, PAIR), f32)],
        scratch=[
            pltpu.VMEM((ROW_LEN, ROW_LEN), f32),
            pltpu.VMEM((24, ROW_LEN), f32),
            pltpu.VMEM((16, ROW_LEN), f32),
            pltpu.VMEM((EMB, HALF), f32),
        ],
        flops=20 * ROW_LEN * ROW_LEN * EMB,
    )


def row_layout(lengths):
    ends = jnp.cumsum(lengths)
    places = jnp.arange(ROW_LEN, dtype=jnp.int32)
    after = places[:, None] >= ends[None, :]
    segment = jnp.sum(after.astype(jnp.int32), axis=1)
    starts = jnp.sum(jnp.where(after, lengths[None, :], 0), axis=1)
    return (segment, places - starts)


def adamw_update(master, moments, grad, factor, rate, step_f):
    scaled = grad * factor
    moment_one = 0.9 * moments[0] + 0.1 * scaled
    moment_two = 0.95 * moments[1] + 0.05 * scaled * scaled
    one_hat = moment_one / (1.0 - jnp.power(0.9, step_f))
    two_hat = moment_two / (1.0 - jnp.power(0.95, step_f))
    updated = master - rate * (one_hat / (jnp.sqrt(two_hat) + 1e-08) + 0.01 * master)
    return (updated, moment_one, moment_two)


def adam_kernel(rate, turned, k_ref, w_ref, m_ref, v_ref, g0_ref, g1_ref, wo_ref, mo_ref, vo_ref):
    grad = jnp.where(pl.program_id(0) == 0, g0_ref[...].astype(f32), g1_ref[...].astype(f32))
    if turned:
        grad = grad.T
    scale_grad = k_ref[0:1, 1:2]
    norm = jnp.sqrt(k_ref[0:1, 0:1] + scale_grad * scale_grad + 1e-06)
    grad = (grad * (clip_limit / jnp.maximum(norm, clip_limit))).reshape(w_ref.shape)
    one = 0.9 * m_ref[...].reshape(w_ref.shape) + 0.1 * grad
    two = 0.95 * v_ref[...].reshape(w_ref.shape) + 0.05 * grad * grad
    w = w_ref[...]
    one_hat = one * (1.0 / (1.0 - 0.9 ** STEP))
    two_hat = two * (1.0 / (1.0 - 0.95 ** STEP))
    wo_ref[...] = w - rate * (one_hat / (jnp.sqrt(two_hat) + 1e-08) + 0.01 * w)
    mo_ref[...] = one
    vo_ref[...] = two


def adam_step(factor, master, moments, grads, tiles, block, where_of, grad_block, grad_at, rate, turned=False):
    spec = pl.BlockSpec((1,) + block, lambda l, t: (l,) + where_of(t))
    first = pl.BlockSpec((1, 1) + block, lambda l, t: (0, l) + where_of(t))
    second = pl.BlockSpec((1, 1) + block, lambda l, t: (1, l) + where_of(t))
    at_zero, at_one = grad_at
    return call(
        functools.partial(adam_kernel, rate, turned),
        (factor, master, moments, moments, *grads),
        [
            whole((8, PAIR)), spec, first, second,
            pl.BlockSpec(grad_block, lambda l, t: (0, at_zero + t)),
            pl.BlockSpec(grad_block, lambda l, t: (0, at_one + t)),
        ],
        [(master.shape, f32)] * 3,
        out_specs=[spec] * 3,
        grid=(LAYERS, tiles),
        flops=20 * master.size,
    )


def swap(values, axis, bit):
    count = lax.axis_size(axis)
    return lax.ppermute(values, axis, [(i, i ^ bit) for i in range(count)])


def bit_orders(axis):
    count = lax.axis_size(axis).bit_length() - 1
    return list(range(count)), list(range(1, count)) + [0]


def swap_core(values, pieces=2):
    parts = jnp.split(values, pieces, axis=0)
    return jnp.concatenate([swap(part, "mp", 1) for part in parts], axis=0)


def gather_rows(values, axis, order):
    index = lax.axis_index(axis)
    share = values.shape
    for bit in order:
        other = swap(values, axis, 1 << bit)
        high = ((index >> bit) & 1) == 1
        values = jnp.stack([jnp.where(high, other, values), jnp.where(high, values, other)])
    done = list(reversed(order))
    count = len(order)
    turn = [done.index(bit) for bit in reversed(range(count))]
    values = values.transpose(turn + [count, count + 1])
    return values.reshape((-1,) + share[1:])


def gather_both(values, axis):
    first, second = bit_orders(axis)
    cut = (values.shape[1] // 2 + PAIR - 1) // PAIR * PAIR
    parts = [
        gather_rows(values[:, :cut], axis, first[::-1]),
        gather_rows(values[:, cut:], axis, second[::-1]),
    ]
    return jnp.concatenate(parts, axis=1)


class Scatter:

    def __init__(self, values, axis, cut=None):
        orders = bit_orders(axis)
        count = len(orders[0])
        self.axis, self.index, self.steps = axis, lax.axis_index(axis), count
        cut = values.shape[1] // 2 if cut is None else cut
        parts = (values[:, :cut], values[:, cut:])
        self.parts = [p.reshape((2,) * count + (-1, p.shape[1])) for p in parts]
        self.left = [list(order) for order in orders]

    def send(self):
        self.kept, self.came = [], []
        for values, left in zip(self.parts, self.left):
            bit = left[0]
            high = ((self.index >> bit) & 1) == 1
            at = sum(1 for other in left if other > bit)
            low_part = lax.index_in_dim(values, 0, at, keepdims=False)
            high_part = lax.index_in_dim(values, 1, at, keepdims=False)
            self.kept.append(jnp.where(high, high_part, low_part))
            self.came.append(swap(jnp.where(high, low_part, high_part), self.axis, 1 << bit))

    def wait_with(self, other):
        first, second, other = lax.optimization_barrier((self.came[0], self.came[1], other))
        self.came = [first, second]
        return other

    def add(self):
        self.left = [left[1:] for left in self.left]
        parts = [k.astype(f32) + c.astype(f32) for k, c in zip(self.kept, self.came)]
        self.parts = parts if not self.left[0] else [p.astype(bf16) for p in parts]

    def result(self):
        return jnp.concatenate(self.parts, axis=1)


def sum_all(values):
    for axis in ("mp", "dp"):
        bit = 1
        while bit < lax.axis_size(axis):
            values = values + swap(values, axis, bit)
            bit *= 2
    return values


def body(
    hidden_in,
    seg_lengths,
    partner,
    qkv_weight,
    out_weight,
    up_weight,
    down_weight,
    norm_params,
    emb_weight,
    log_scale,
    qkv_moments,
    out_moments,
    up_moments,
    down_moments,
    norm_moments,
    emb_moments,
    scale_moments,
):
    share = qkv_weight.shape[1]
    mp_count = lax.axis_size("mp")
    place = lax.axis_index("mp")
    core = place & 1
    far_chip = (place >> 1) == 1
    core_arr = core.reshape(1).astype(jnp.int32)

    def mine(first, second):
        return jnp.where(far_chip, second, first)

    def attn_pack(layer_at):
        return [qkv_weight[layer_at].reshape(share, 3 * WIDE), out_weight[layer_at].T]

    def mlp_pack(layer_at):
        return [up_weight[layer_at], down_weight[layer_at].T]

    norm_cols = jnp.pad(norm_params.reshape(4 * LAYERS, share).T, ((0, 0), (0, PAIR - 4 * LAYERS)))

    def packed(parts):
        return jnp.concatenate(parts, axis=1).astype(bf16)

    def gather(values):
        return lax.all_gather(values, "dp", axis=0, tiled=True)

    first_w = gather_both(packed(attn_pack(0) + [norm_cols]), "dp")
    middle_w = gather(packed(attn_pack(1) + mlp_pack(0)))
    last_w = gather(packed(mlp_pack(1) + [emb_weight]))
    attn_w = [first_w, middle_w]
    mlp_w = [(middle_w, 1), (last_w, 0)]
    nrm = first_w[:, 4 * WIDE : 4 * WIDE + 4 * LAYERS].T.astype(f32)
    w_emb = last_w[:, 2 * HID :]

    segment, offset = row_layout(seg_lengths[0])

    def own_order(values):
        blocks = values.reshape(2, 2, BLK)
        return jnp.where(core == 1, blocks[:, ::-1], blocks).reshape(ROW_LEN)

    segment = own_order(segment).astype(f32)
    offset = own_order(offset).astype(f32)
    seg_col = jnp.broadcast_to(segment[:, None], (ROW_LEN, PAIR))
    seg_row = jnp.broadcast_to(segment[None, :], (8, ROW_LEN))
    lane = jnp.arange(PAIR, dtype=jnp.int32)
    frequency = jnp.exp((lane % (HEAD_DIM // 2)).astype(f32) * (-2.0 * math.log(10000.0) / HEAD_DIM))
    angles = offset[:, None] * frequency[None, :]
    cosines = jnp.cos(angles)
    sines = jnp.where((lane % HEAD_DIM) < HEAD_DIM // 2, -1.0, 1.0)[None, :] * jnp.sin(angles)

    other_half = swap(hidden_in, "mp", 2)
    low = [mine(hidden_in, other_half), mine(other_half, hidden_in)]
    stream = [v.astype(f32) for v in low]

    def chip_sum(own, send):
        return (own.astype(f32) + swap_core(send).astype(f32)).astype(bf16)

    def cross(total, earlier=None):
        if earlier is not None:
            total, earlier = lax.optimization_barrier((total, earlier))
        return total, swap(total, "mp", 2), earlier

    kept = []
    sums = None
    for layer_at in range(LAYERS):
        streams, qkvs, norm_prev = [], [], []
        if layer_at > 0:
            stream, low = [], []
        for at in range(2):
            if layer_at > 0:
                h, hb, zz = norm_fwd(4 * layer_at - 2, normed[at], *sums[at], nrm)
                stream.append(h)
                low.append(hb)
                kept[-1][-1].append(zz)
            sib = swap_core(low[at])
            streams += [low[at], sib]
            qkvs.append(qkv_project(low[at], sib, attn_w[layer_at], cosines, sines, at))
        o_a, lse_a, own, send = attend(
            0, core_arr, qkvs[0], qkvs[1], seg_col, seg_row, attn_w[layer_at], None
        )
        total_a, came_a, _ = cross(chip_sum(own, send))
        o_b, lse_b, own, send = attend(
            1, core_arr, qkvs[1], qkvs[0], seg_col, seg_row, attn_w[layer_at], total_a
        )
        total_b, came_b, came_a = cross(chip_sum(own, send), came_a)
        h_a, hb_a, z_a = norm_fwd(4 * layer_at, stream[0], total_a, came_a, nrm)
        sib_a = swap_core(hb_a)
        zg_a, own, send = mlp(hb_a, sib_a, mlp_w[layer_at], None)
        next_a, next_came_a, came_b = cross(chip_sum(own, send), came_b)
        h_b, hb_b, z_b = norm_fwd(4 * layer_at, stream[1], total_b, came_b, nrm)
        sib_b = swap_core(hb_b)
        zg_b, own, send = mlp(hb_b, sib_b, mlp_w[layer_at], None)
        next_b, next_came_b, next_came_a = cross(chip_sum(own, send), next_came_a)
        normed = [h_a, h_b]
        sums = [(next_a, next_came_a), (next_b, next_came_b)]
        kept.append(
            (streams, qkvs, [(o_a, lse_a), (o_b, lse_b)], [z_a, z_b], [hb_a, sib_a, hb_b, sib_b], [zg_a, zg_b], [])
        )
    stream, low = [], []
    for at in range(2):
        h, hb, zz = norm_fwd(4 * LAYERS - 2, normed[at], *sums[at], nrm)
        stream.append(h)
        low.append(hb)
        kept[-1][-1].append(zz)
    hidden_out = mine(stream[0], stream[1])

    emb_own = jnp.concatenate([dot_nn(low[0], w_emb), dot_nn(low[1], w_emb)], axis=0).astype(bf16)
    emb_all = jnp.concatenate([emb_own, swap(emb_own, "mp", 1)], axis=0)

    def loss_order(values):
        return values.reshape(2, 2, BLK).transpose(1, 0, 2).reshape(ROW_LEN)

    loss_seg = loss_order(segment)
    lengths = jnp.broadcast_to(
        jnp.pad(seg_lengths[0].astype(f32), (0, PAIR - SEGS), constant_values=1.0)[None], (8, PAIR)
    )
    partners = jnp.broadcast_to(
        jnp.pad(partner[0].astype(f32), (0, PAIR - SEGS), constant_values=-1.0)[None], (8, PAIR)
    )
    dx0, dx1, g_emb, loss_parts = loss_and_grads(
        log_scale,
        emb_all,
        jnp.broadcast_to(loss_seg[:, None], (ROW_LEN, PAIR)),
        jnp.broadcast_to(loss_seg[None, :], (8, ROW_LEN)),
        lengths,
        partners,
        low[0],
        low[1],
        w_emb,
    )

    grads = [dx0, dx1]
    pending = [(), ()]
    reduced = []
    norm_grads = [None] * LAYERS
    for layer_at in reversed(range(LAYERS)):
        streams, qkvs, attended, norm_a, hiddens, zgs, norm_b = kept[layer_at]
        row = 4 * layer_at + 2
        d_a, db_a, gain_a = norm_bwd(row, grads[0], pending[0], norm_b[0], nrm)
        sib_a = swap_core(db_a)
        du_a, own, send = mlp_back(db_a, sib_a, zgs[0], mlp_w[layer_at], None)
        total_a = chip_sum(own, send)
        if pending[1]:
            total_a, came_a, came_b = cross(total_a, pending[1][1])
            if upper.left[0]:
                came_b = upper.wait_with(came_b)
                upper.add()
                upper.send()
            pending[1] = (pending[1][0], came_b)
        else:
            total_a, came_a, _ = cross(total_a)
        d_b, db_b, gain_b = norm_bwd(row, grads[1], pending[1], norm_b[1], nrm)
        sib_b = swap_core(db_b)
        du_b, own, send = mlp_back(db_b, sib_b, zgs[1], mlp_w[layer_at], total_a)
        total_b, came_b, came_a = cross(chip_sum(own, send), came_a)
        gains = [(gain_a + gain_b)[:2]]
        both = mlp_grads(hiddens, [db_a, sib_a, db_b, sib_b], [du_a, du_b], zgs, total_b)
        both, came_b = lax.optimization_barrier((both, came_b))
        reduced.append(lax.psum_scatter(both, "dp", scatter_dimension=0, tiled=True))
        row = 4 * layer_at
        grad_a, low_a, gain_a = norm_bwd(row, d_a, (total_a, came_a), norm_a[0], nrm)
        sib_a = swap_core(low_a)
        if layer_at < LAYERS - 1:
            came_b = upper.wait_with(came_b)
            upper.add()
            upper.send()
        grad_b, low_b, gain_b = norm_bwd(row, d_b, (total_b, came_b), norm_a[1], nrm)
        dattn = [low_a, sib_a, low_b, swap_core(low_b)]
        dmixes = attend_back(
            core_arr, dattn, attn_w[layer_at], *qkvs, attended[0][0], attended[1][0],
            attended[0][1], attended[1][1], seg_col, seg_row, cosines, sines,
        )
        norm_grads[layer_at] = jnp.concatenate([(gain_a + gain_b)[:2]] + gains, axis=0)
        outs = [attended[0][0], attended[1][0]]
        grads = [grad_a, grad_b]
        if layer_at > 0:
            total_a, came_a, _ = cross(chip_sum(*qkv_back(dmixes[0], attn_w[layer_at], None)))
            above = attn_grads(streams, dattn, dmixes, outs, total_a)
            above, came_a = lax.optimization_barrier((above, came_a))
            upper = Scatter(above, "dp")
            upper.send()
            total_b, came_b, came_a = cross(
                chip_sum(*qkv_back(dmixes[1], attn_w[layer_at], total_a)), came_a
            )
            pending = [(total_a, came_a), (total_b, came_b)]
        else:
            norm_rows = jnp.concatenate(norm_grads, axis=0)
            small = jnp.concatenate([g_emb, jnp.pad(norm_rows.T, ((0, 0), (0, PAIR - 4 * LAYERS)))], axis=1)
            last = attn_grads(streams, dattn, dmixes, outs, None, small.astype(bf16))
            lower = Scatter(last, "dp")
            squares = jnp.sum(jnp.square(reduced[0].astype(f32)))
            while lower.left[0]:
                lower.send()
                if len(lower.left[0]) == lower.steps:
                    squares = upper.wait_with(lower.wait_with(squares))
                    while upper.left[0]:
                        upper.add()
                        if upper.left[0]:
                            upper.send()
                    fourth = upper.result()
                    squares = squares + jnp.sum(jnp.square(fourth))
                lower.add()
            third = lower.result()
            totals = []
            for at in range(2):
                own, send = qkv_back(dmixes[at], attn_w[layer_at], last)
                totals.append(own.astype(f32) + swap(send, "mp", 1).astype(f32))
            came = swap(mine(totals[1], totals[0]).astype(bf16), "mp", 2)
            hidden_grad = mine(grads[0], grads[1]) + (mine(totals[0], totals[1]) + came.astype(f32))

    first, second = reduced
    third, hidden_grad = lax.optimization_barrier((third, hidden_grad))
    small = third[:, 4 * WIDE :]
    small = small + swap(small, "mp", 1)
    emb_grad = small[:, :EMB]
    norm_grad = small[:, EMB : EMB + 4 * LAYERS].T.reshape(LAYERS, 2, 2, share)
    squares = (
        squares + jnp.sum(jnp.square(second.astype(f32))) + jnp.sum(jnp.square(third[:, : 4 * WIDE]))
        + jnp.sum(small * small) / mp_count
    )
    parts = jnp.concatenate([loss_parts[:2], jnp.zeros((6, PAIR), f32)], axis=0)
    loss_here = jnp.sum(parts[0]) / mp_count
    dscale_here = jnp.sum(parts[1]) / mp_count
    vector = jnp.where(lane == 0, squares, jnp.where(lane == 1, dscale_here, jnp.where(lane == 2, loss_here, 0.0)))
    vector = sum_all(jnp.broadcast_to(vector[None], (8, PAIR)))
    total_squares = vector[0, 0]
    scale_grad = vector[0, 1:2]
    loss_total = vector[0, 2]
    norm_value = jnp.sqrt(total_squares + scale_grad[0] * scale_grad[0] + 1e-06)
    factor = clip_limit / jnp.maximum(norm_value, clip_limit)
    step_f = jnp.asarray(STEP, f32)
    qkv_step = adam_step(
        vector, qkv_weight.transpose(0, 2, 1, 3), qkv_moments.transpose(0, 1, 3, 2, 4), (third, fourth),
        3, (1, share, WIDE), lambda t: (t, 0, 0), (share, WIDE), (0, 0), D ** (-0.5),
    )
    qkv_new, qkv_first, qkv_second = [v.transpose(0, 2, 1, 3) for v in qkv_step]
    out_new, out_first, out_second = adam_step(
        vector, out_weight, out_moments, (third, fourth),
        1, (WIDE, share), lambda t: (t, 0), (share, WIDE), (3, 3), (D * SEGS // ROW_LEN) ** (-0.5), True,
    )
    up_new, up_first, up_second = adam_step(
        vector, up_weight, up_moments, (second, first),
        2, (share, HALF), lambda t: (0, t), (share, HALF), (0, 0), D ** (-0.5),
    )
    down_new, down_first, down_second = adam_step(
        vector, down_weight, down_moments, (second, first),
        4, (TILE, share), lambda t: (t, 0), (share, TILE), (4, 4), FF ** (-0.5), True,
    )
    norm_new, norm_first, norm_second = adamw_update(norm_params, norm_moments, norm_grad, factor, 0.5, step_f)
    emb_new, emb_first, emb_second = adamw_update(emb_weight, emb_moments, emb_grad, factor, D ** (-0.5), step_f)
    scale_new, scale_first, scale_second = adamw_update(log_scale, scale_moments, scale_grad, factor, 1.0, step_f)
    return (
        hidden_out,
        hidden_grad,
        loss_total.reshape(1),
        norm_value.reshape(1),
        qkv_new,
        qkv_first,
        qkv_second,
        out_new,
        out_first,
        out_second,
        up_new,
        up_first,
        up_second,
        down_new,
        down_first,
        down_second,
        norm_new,
        norm_first,
        norm_second,
        emb_new,
        emb_first,
        emb_second,
        scale_new,
        scale_first,
        scale_second,
    )


def solution(mesh):
    placed = (
        P(("dp", "mp"), None),
        P("dp", None),
        P("dp", None),
        P(None, "dp", None, "mp"),
        P(None, "mp", "dp"),
        P(None, "dp", "mp"),
        P(None, "mp", "dp"),
        P(None, None, None, "dp"),
        P("dp", None),
        P(),
        P(None, None, "dp", None, "mp"),
        P(None, None, "mp", "dp"),
        P(None, None, "dp", "mp"),
        P(None, None, "mp", "dp"),
        P(None, None, None, None, "dp"),
        P(None, "dp", None),
        P(),
    )
    results = (P(("dp", "mp"), None), P(("dp", "mp"), None), P(), P())
    for at in (3, 4, 5, 6, 7, 8, 9):
        results += (placed[at],) * 3
    return jax.shard_map(body, mesh=mesh, in_specs=placed, out_specs=results, check_vma=False)
```

```python
import functools
import math

import jax
import jax.numpy as jnp
from jax import lax
from jax.experimental import pallas as pl
from jax.experimental.pallas import tpu as pltpu
from jax.sharding import PartitionSpec as P

D = 1024
HEAD_DIM = 64
FF = 4096
EMB = 128
LAYERS = 2
STEP = 5
ROW_LEN = 1024
SEGS = 8

BLK = 256
HALF = 512
WIDE = 256
HID = 1024
PAIR = 128
PAIRS = WIDE // PAIR
MIB = 1 << 20
COST = 1

f32 = jnp.float32
bf16 = jnp.bfloat16
best = lax.Precision.HIGHEST
sharpness = 0.05
clip_limit = 1.0

OUT_AT = 3 * WIDE


def dot_nn(left, right):
    return lax.dot_general(left, right, (((1,), (0,)), ((), ())), preferred_element_type=f32)


def dot_nt(left, right):
    return lax.dot_general(left, right, (((1,), (1,)), ((), ())), preferred_element_type=f32)


def dot_tn(left, right):
    return lax.dot_general(left, right, (((0,), (0,)), ((), ())), preferred_element_type=f32)


def whole(shape):
    return pl.BlockSpec(shape, lambda *_: (0,) * len(shape))


def call(kernel, args, in_specs, outs, out_specs=None, grid=(1,), scratch=(), flops=0, vmem=32, alias=None,
         keep=(), after=None, far=()):
    out_shape = [
        pltpu.HBM(s, d) if i in keep else jax.ShapeDtypeStruct(s, d) for i, (s, d) in enumerate(outs)
    ]
    if out_specs is None:
        out_specs = [whole(s) for s, _ in outs]
    args = [pltpu.with_memory_space_constraint(a, pltpu.HBM) if i in far else a for i, a in enumerate(args)]
    in_specs = list(in_specs)
    moved = sum(math.prod(a.shape) * a.dtype.itemsize for a in args if a.size < 3 * MIB)
    moved += sum(math.prod(s) * jnp.dtype(d).itemsize for s, d in outs)
    body_fn = kernel
    if after is not None:
        count = len(args)
        args = args + [after]
        in_specs = in_specs + [pl.BlockSpec(memory_space=pl.ANY)]

        def body_fn(*refs):
            kernel(*refs[:count], *refs[count + 1 :])

    return pl.pallas_call(
        body_fn,
        grid=grid,
        in_specs=in_specs,
        out_specs=out_specs,
        out_shape=out_shape,
        scratch_shapes=list(scratch),
        input_output_aliases=alias or {},
        compiler_params=pltpu.CompilerParams(
            dimension_semantics=("arbitrary",) * len(grid), vmem_limit_bytes=vmem * MIB
        ),
        cost_estimate=pl.CostEstimate(flops=int(flops * COST), bytes_accessed=int(moved * COST), transcendentals=0),
    )(*args)


def smem():
    return pl.BlockSpec(memory_space=pltpu.SMEM)


def halves(values):
    high = values.astype(bf16)
    return high, (values - high.astype(f32)).astype(bf16)


def norm_fwd_kernel(row, with_sums, *refs):
    if with_sums:
        x_ref, s_ref, r_ref, n_ref, h_ref, hb_ref, z_ref = refs
        v = x_ref[...].astype(f32) + (s_ref[...].astype(f32) + r_ref[...].astype(f32))
    else:
        x_ref, n_ref, h_ref, hb_ref, z_ref = refs
        v = x_ref[...].astype(f32)
    cen = v - jnp.mean(v, axis=1, keepdims=True)
    var = jnp.mean(cen * cen, axis=1, keepdims=True)
    rstd = lax.rsqrt(var + 1e-05)
    z = cen * rstd
    h = z * n_ref[row : row + 1, :] + n_ref[row + 1 : row + 2, :]
    h_ref[...] = h
    hb_ref[...] = h.astype(bf16)
    z_ref[:, 0:D] = z.astype(bf16)
    high, rest = halves(rstd)
    lane = lax.broadcasted_iota(jnp.int32, (BLK, PAIR), 1)
    z_ref[:, D:] = jnp.where(lane < 1, high.astype(f32), rest.astype(f32)).astype(bf16)


def norm_fwd(row, x, s, r, nrm):
    blk = whole((BLK, D))
    return call(
        functools.partial(norm_fwd_kernel, row, True),
        (x, s, r, nrm),
        [blk, blk, blk, whole(nrm.shape)],
        [((BLK, D), f32), ((BLK, D), bf16), ((BLK, D + PAIR), bf16)],
        flops=BLK * D * 10,
        keep=(2,),
    )


def norm_bwd_kernel(row, with_sums, *refs):
    if with_sums:
        d_ref, s_ref, r_ref, z_ref, n_ref, o_ref, ob_ref, g_ref = refs
        dy = d_ref[...] + (s_ref[...].astype(f32) + r_ref[...].astype(f32))
    else:
        d_ref, z_ref, n_ref, o_ref, ob_ref, g_ref = refs
        dy = d_ref[...]
    z = z_ref[:, 0:D].astype(f32)
    rstd = z_ref[:, D : D + 1].astype(f32) + z_ref[:, D + 1 : D + 2].astype(f32)
    dz = dy * n_ref[row : row + 1, :]
    m1 = jnp.mean(dz, axis=1, keepdims=True)
    m2 = jnp.mean(dz * z, axis=1, keepdims=True)
    dr = (dz - m1 - z * m2) * rstd
    o_ref[...] = dr
    ob_ref[...] = dr.astype(bf16)
    g_ref[...] = jnp.concatenate(
        [jnp.sum(dy * z, axis=0, keepdims=True), jnp.sum(dy, axis=0, keepdims=True), jnp.zeros((6, D), f32)],
        axis=0,
    )


def norm_bwd(row, d, sums, z, nrm):
    blk = whole((BLK, D))
    args = (d,) + tuple(sums) + (z, nrm)
    return call(
        functools.partial(norm_bwd_kernel, row, len(sums) > 0),
        args,
        [blk] * (1 + len(sums)) + [whole((BLK, D + PAIR)), whole(nrm.shape)],
        [((BLK, D), f32), ((BLK, D), bf16), ((8, D), f32)],
        flops=BLK * D * 14,
        far=(1 + len(sums),),
    )


def rope_lanes(values, cosines, sines):
    lane = lax.broadcasted_iota(jnp.int32, values.shape, 1)
    low = (lane & (HEAD_DIM - 1)) < HEAD_DIM // 2
    swapped = jnp.where(
        low, pltpu.roll(values, PAIR - HEAD_DIM // 2, 1), pltpu.roll(values, HEAD_DIM // 2, 1)
    )
    return values * cosines + swapped * sines


def qkv_kernel(xo_ref, xs_ref, w_ref, c_ref, s_ref, m_ref):
    for at, x_ref in enumerate((xo_ref, xs_ref)):
        rows = slice(at * BLK, (at + 1) * BLK)
        mix = dot_nn(x_ref[...], w_ref[...])
        cosines, sines = c_ref[rows, :], s_ref[rows, :]
        for p in range(PAIRS):
            lanes = slice(p * PAIR, (p + 1) * PAIR)
            q = rope_lanes(mix[:, p * PAIR : (p + 1) * PAIR], cosines, sines).astype(bf16)
            m_ref[rows, lanes] = q * HEAD_DIM ** (-0.5)
            lanes = slice(WIDE + p * PAIR, WIDE + (p + 1) * PAIR)
            m_ref[rows, lanes] = rope_lanes(mix[:, lanes], cosines, sines).astype(bf16)
        m_ref[rows, 2 * WIDE :] = mix[:, 2 * WIDE :].astype(bf16)


def qkv_project(x_own, x_sib, weights, cosines, sines, at):
    blk = whole((BLK, D))
    tab = pl.BlockSpec((HALF, PAIR), lambda *_: (at, 0))
    return call(
        qkv_kernel,
        (x_own, x_sib, weights, cosines, sines),
        [blk, blk, pl.BlockSpec((D, 3 * WIDE), lambda *_: (0, 0)), tab, tab],
        [((HALF, 3 * WIDE), bf16)],
        flops=2 * HALF * D * 3 * WIDE,
        keep=(0,),
    )[0]


def near_places(core, at):
    if at == 0:
        return 1 - core, core
    return core, 1 - core


def attend_kernel(at, core_ref, m_ref, mo_ref, sc_ref, sco_ref, sr_ref, w_ref, o_ref, l_ref, own_ref, send_ref):
    q_ref, k_ref, v_ref = [m_ref.at[:, i * WIDE : (i + 1) * WIDE] for i in range(3)]
    ko_ref, vo_ref = [mo_ref.at[:, i * WIDE : (i + 1) * WIDE] for i in (1, 2)]
    near, cross = near_places(core_ref[0], at)
    cross_rows = pl.ds(pl.multiple_of(cross * BLK, BLK), BLK)
    row_at = lax.broadcasted_iota(jnp.int32, (PAIR, BLK), 0)
    lane_at = lax.broadcasted_iota(jnp.int32, (BLK, PAIR), 1)
    seg_main = sc_ref[...]
    seg_main = jnp.concatenate([seg_main, seg_main], axis=1)
    seg_cross = sco_ref[cross_rows, :]
    seg_cross = jnp.concatenate([seg_cross, seg_cross], axis=1)
    l_ref[...] = jnp.zeros(l_ref.shape, f32)
    for is_near in (False, True):
        place = near if is_near else 1 - near
        start = pl.multiple_of(place * BLK, BLK)
        rows = pl.ds(start, BLK)
        seg_q = sr_ref[0:1, rows]
        bias = jnp.where(seg_main == seg_q, 0.0, -1e30)
        if is_near:
            bias_cross = jnp.where(seg_cross == seg_q, 0.0, -1e30)
        for p in range(PAIRS):
            lanes = slice(p * PAIR, (p + 1) * PAIR)
            keys = k_ref[:, lanes]
            values_t = v_ref[:, lanes].T
            queries = q_ref[rows, lanes]
            if is_near:
                keys_cross = ko_ref[cross_rows, lanes]
                values_cross_t = vo_ref[cross_rows, lanes].T
            parts = []
            for h in range(2):
                q = jnp.where((lane_at >= HEAD_DIM) == (h == 1), queries, jnp.zeros_like(queries))
                scores = dot_nt(keys, q) + bias
                top = jnp.max(scores, axis=0, keepdims=True)
                if is_near:
                    scores_cross = dot_nt(keys_cross, q) + bias_cross
                    top = jnp.maximum(top, jnp.max(scores_cross, axis=0, keepdims=True))
                e = jnp.exp(scores - top)
                total = jnp.sum(e, axis=0, keepdims=True)
                mixed = dot_nn(values_t, e.astype(bf16))
                if is_near:
                    e = jnp.exp(scores_cross - top)
                    total = total + jnp.sum(e, axis=0, keepdims=True)
                    mixed = mixed + dot_nn(values_cross_t, e.astype(bf16))
                parts.append(mixed / total)
                head = 2 * p + h
                l_ref[head : head + 1, rows] = top + jnp.log(total)
            both = jnp.where(row_at < HEAD_DIM, parts[0], parts[1])
            o_ref[rows, lanes] = both.T.astype(bf16)
    own_ref[...] = dot_nt(o_ref[0:BLK, :], w_ref[...]).astype(bf16)
    send_ref[...] = dot_nt(o_ref[BLK:HALF, :], w_ref[...]).astype(bf16)


def attend(at, core, qkv, qkv_other, seg_col, seg_row, weights, after):
    mix = whole((HALF, 3 * WIDE))
    return call(
        functools.partial(attend_kernel, at),
        (core, qkv, qkv_other, seg_col, seg_col, seg_row, weights),
        [
            smem(), mix, mix,
            pl.BlockSpec((HALF, PAIR), lambda *_: (at, 0)),
            pl.BlockSpec((HALF, PAIR), lambda *_: (1 - at, 0)),
            pl.BlockSpec((8, HALF), lambda *_: (0, at)),
            pl.BlockSpec((D, WIDE), lambda *_: (0, OUT_AT // WIDE)),
        ],
        [((HALF, WIDE), bf16), ((8, HALF), f32), ((BLK, D), bf16), ((BLK, D), bf16)],
        flops=4 * 4 * 5 * BLK * BLK * PAIR + 2 * HALF * WIDE * D,
        far=(1, 2),
        keep=(0, 1),
        after=after,
    )


def attend_back_kernel(core_ref, d0o, d0s, d1o, d1s, w_ref, mix0, mix1, o0, o1, l0, l1,
                       sc_ref, sr_ref, c_ref, s_ref, m0_ref, m1_ref,
                       dout_ref, dk_ref, dv_ref, dq_ref):
    for i, d in enumerate((d0o, d0s, d1o, d1s)):
        dout_ref[i // 2, (i % 2) * BLK : (i % 2 + 1) * BLK, :] = dot_nn(d[...], w_ref[...]).astype(bf16)
    dk_ref[...] = jnp.zeros(dk_ref.shape, f32)
    dv_ref[...] = jnp.zeros(dv_ref.shape, f32)
    row_at = lax.broadcasted_iota(jnp.int32, (PAIR, 1), 0)
    lane_at = lax.broadcasted_iota(jnp.int32, (1, PAIR), 1)
    scaling = HEAD_DIM ** (-0.5)
    q_refs, k_refs, v_refs = [
        [m.at[:, i * WIDE : (i + 1) * WIDE] for m in (mix0, mix1)] for i in range(3)
    ]
    o_refs, l_refs = (o0, o1), (l0, l1)
    for at in range(2):
        near, cross = near_places(core_ref[0], at)
        cross_rows = pl.ds(pl.multiple_of(cross * BLK, BLK), BLK)
        cross_full = pl.ds(pl.multiple_of((1 - at) * HALF + cross * BLK, BLK), BLK)
        seg_main = sc_ref[at * HALF : (at + 1) * HALF, :]
        seg_main = jnp.concatenate([seg_main, seg_main], axis=1)
        seg_cross = sc_ref[cross_full, :]
        seg_cross = jnp.concatenate([seg_cross, seg_cross], axis=1)
        for is_near in (False, True):
            place = near if is_near else 1 - near
            rows = pl.ds(pl.multiple_of(place * BLK, BLK), BLK)
            seg_q = sr_ref[0:1, pl.ds(pl.multiple_of(at * HALF + place * BLK, BLK), BLK)]
            bias = jnp.where(seg_main == seg_q, 0.0, -1e30)
            if is_near:
                bias_cross = jnp.where(seg_cross == seg_q, 0.0, -1e30)
            for p in range(PAIRS):
                lanes = slice(p * PAIR, (p + 1) * PAIR)
                keys, values = k_refs[at][:, lanes], v_refs[at][:, lanes]
                keys_t = keys.T
                queries, douts = q_refs[at][rows, lanes], dout_ref[at, rows, lanes]
                if is_near:
                    keys_cross = k_refs[1 - at][cross_rows, lanes]
                    values_cross = v_refs[1 - at][cross_rows, lanes]
                    keys_cross_t = keys_cross.T
                products = (douts.astype(f32) * o_refs[at][rows, lanes].astype(f32)).T
                dq_t = jnp.zeros((PAIR, BLK), f32)
                for h in range(2):
                    in_lanes = (lane_at >= HEAD_DIM) == (h == 1)
                    in_rows = (row_at >= HEAD_DIM) == (h == 1)
                    q = jnp.where(in_lanes, queries, jnp.zeros_like(queries))
                    d = jnp.where(in_lanes, douts, jnp.zeros_like(douts))
                    delta = jnp.sum(products[h * HEAD_DIM : (h + 1) * HEAD_DIM, :], axis=0, keepdims=True)
                    lse = l_refs[at][2 * p + h : 2 * p + h + 1, rows]
                    kt = jnp.where(in_rows, keys_t, jnp.zeros_like(keys_t))
                    probs = jnp.exp(dot_nt(keys, q) + bias - lse)
                    dscores = (probs * (dot_nt(values, d) - delta)).astype(bf16)
                    dv_ref[at, :, lanes] += dot_nn(probs.astype(bf16), d)
                    dk_ref[at, :, lanes] += dot_nn(dscores, q)
                    dq_t = dq_t + dot_nn(kt, dscores)
                    if is_near:
                        kt = jnp.where(in_rows, keys_cross_t, jnp.zeros_like(keys_cross_t))
                        probs = jnp.exp(dot_nt(keys_cross, q) + bias_cross - lse)
                        dscores = (probs * (dot_nt(values_cross, d) - delta)).astype(bf16)
                        dv_ref[1 - at, cross_rows, lanes] += dot_nn(probs.astype(bf16), d)
                        dk_ref[1 - at, cross_rows, lanes] += dot_nn(dscores, q)
                        dq_t = dq_t + dot_nn(kt, dscores)
                dq_ref[at, rows, lanes] = dq_t.T * scaling
    for at, m_ref in enumerate((m0_ref, m1_ref)):
        rows = slice(at * HALF, (at + 1) * HALF)
        cosines, sines = c_ref[rows, :], -s_ref[rows, :]
        for p in range(PAIRS):
            lanes = slice(p * PAIR, (p + 1) * PAIR)
            m_ref[:, p * PAIR : (p + 1) * PAIR] = rope_lanes(dq_ref[at, :, lanes], cosines, sines).astype(bf16)
            m_ref[:, WIDE + p * PAIR : WIDE + (p + 1) * PAIR] = rope_lanes(
                dk_ref[at, :, lanes], cosines, sines
            ).astype(bf16)
        m_ref[:, 2 * WIDE :] = dv_ref[at].astype(bf16)


def attend_back(core, dblocks, weights, qkv_a, qkv_b, o_a, o_b, l_a, l_b, seg_col, seg_row, cosines, sines):
    blk, half, low, mix = whole((BLK, D)), whole((HALF, WIDE)), whole((8, HALF)), whole((HALF, 3 * WIDE))
    tab = whole((ROW_LEN, PAIR))
    return call(
        attend_back_kernel,
        (core, *dblocks, weights, qkv_a, qkv_b, o_a, o_b, l_a, l_b, seg_col, seg_row, cosines, sines),
        [smem(), blk, blk, blk, blk, pl.BlockSpec((D, WIDE), lambda *_: (0, OUT_AT // WIDE))]
        + [mix, mix, half, half]
        + [low, low, tab, whole((8, ROW_LEN)), tab, tab],
        [((HALF, 3 * WIDE), bf16)] * 2,
        scratch=[
            pltpu.VMEM((2, HALF, WIDE), bf16),
            pltpu.VMEM((2, HALF, WIDE), f32),
            pltpu.VMEM((2, HALF, WIDE), f32),
            pltpu.VMEM((2, HALF, WIDE), f32),
        ],
        flops=10 * 4 * 10 * BLK * BLK * PAIR + 2 * ROW_LEN * WIDE * D,
        far=(6, 7, 8, 9, 10, 11),
    )


def spread_kernel(m_ref, w_ref, own_ref, send_ref):
    own_ref[...] = dot_nt(m_ref[0:BLK, :], w_ref[...]).astype(bf16)
    send_ref[...] = dot_nt(m_ref[BLK:HALF, :], w_ref[...]).astype(bf16)


def qkv_back(dmix, weights, after):
    return call(
        spread_kernel,
        (dmix, weights),
        [whole(dmix.shape), pl.BlockSpec((D, 3 * WIDE), lambda *_: (0, 0))],
        [((BLK, D), bf16)] * 2,
        flops=2 * HALF * D * 3 * WIDE,
        after=after,
    )


TILE = 256
TILES = HID // TILE


def gelu_pair(u):
    half = jnp.exp(u * u * -0.5)
    t = 1.0 / (1.0 + (0.3275911 * 0.5 ** 0.5) * jnp.abs(u))
    poly = t * (
        0.5 * 0.254829592
        + t * (0.5 * -0.284496736 + t * (0.5 * 1.421413741 + t * (0.5 * -1.453152027 + t * (0.5 * 1.061405429))))
    )
    tail = poly * half
    phi = jnp.where(u >= 0.0, 1.0 - tail, tail)
    return u * phi, phi + u * half * (1.0 / math.sqrt(2.0 * math.pi))


def mlp_kernel(ho_ref, hs_ref, up_ref, down_ref, zg_ref, own_ref, send_ref):
    for at, (h_ref, p_ref) in enumerate(((ho_ref, own_ref), (hs_ref, send_ref))):
        rows = slice(at * BLK, (at + 1) * BLK)
        value, slope = gelu_pair(dot_nn(h_ref[...], up_ref[...]))
        z = value.astype(bf16)
        zg_ref[rows, 0:HID] = z
        zg_ref[rows, HID:] = slope.astype(bf16)
        p_ref[...] = dot_nt(z, down_ref[...]).astype(bf16)


def mlp(h_own, h_sib, weights, after):
    blk = whole((BLK, D))
    array, first = weights
    return call(
        mlp_kernel,
        (h_own, h_sib, array, array),
        [
            blk, blk,
            pl.BlockSpec((D, HID), lambda *_: (0, first)),
            pl.BlockSpec((D, HID), lambda *_: (0, first + 1)),
        ],
        [((HALF, 2 * HID), bf16), ((BLK, D), bf16), ((BLK, D), bf16)],
        flops=4 * HALF * D * HID,
        keep=(0,),
        after=after,
    )


def mlp_back_kernel(do_ref, ds_ref, g_ref, up_ref, down_ref, du_ref, own_ref, send_ref):
    for at, (d_ref, p_ref) in enumerate(((do_ref, own_ref), (ds_ref, send_ref))):
        rows = slice(at * BLK, (at + 1) * BLK)
        du = (dot_nn(d_ref[...], down_ref[...]) * g_ref[rows, :].astype(f32)).astype(bf16)
        du_ref[rows, :] = du
        p_ref[...] = dot_nt(du, up_ref[...]).astype(bf16)


def mlp_back(d_own, d_sib, zg, weights, after):
    blk = whole((BLK, D))
    array, first = weights
    return call(
        mlp_back_kernel,
        (d_own, d_sib, zg, array, array),
        [
            blk, blk,
            pl.BlockSpec((HALF, HID), lambda *_: (0, 1)),
            pl.BlockSpec((D, HID), lambda *_: (0, first)),
            pl.BlockSpec((D, HID), lambda *_: (0, first + 1)),
        ],
        [((HALF, HID), bf16), ((BLK, D), bf16), ((BLK, D), bf16)],
        flops=4 * HALF * D * HID,
        far=(2,),
        after=after,
    )


def turn_into(t_ref, x_refs):
    for i, x in enumerate(x_refs):
        t_ref[:, i * BLK : (i + 1) * BLK] = x[...].T


def grad_tile(t_ref, y_refs):
    first, second = y_refs
    return (dot_nn(t_ref[:, 0:HALF], first[...]) + dot_nn(t_ref[:, HALF:], second[...])).astype(bf16)


def mlp_grad_kernel(x0, x1, x2, x3, d0, d1, d2, d3, u0, u1, z0, z1, g_ref, t_ref):
    step = pl.program_id(0)

    @pl.when(step == 0)
    def _():
        turn_into(t_ref, (x0, x1, x2, x3))

    @pl.when(step == HID // HALF)
    def _():
        turn_into(t_ref, (d0, d1, d2, d3))

    @pl.when(step < HID // HALF)
    def _():
        g_ref[...] = grad_tile(t_ref, (u0, u1))

    @pl.when(step >= HID // HALF)
    def _():
        g_ref[...] = grad_tile(t_ref, (z0, z1))


def mlp_grads(hidden, dblocks, dus, zs, after):
    blk = whole((BLK, D))
    tiles = HID // HALF
    first = pl.BlockSpec((HALF, HALF), lambda t: (0, jnp.minimum(t, tiles - 1)))
    second = pl.BlockSpec((HALF, HALF), lambda t: (0, jnp.maximum(t - tiles, 0)))
    return call(
        mlp_grad_kernel,
        (*hidden, *dblocks, *dus, *zs),
        [blk] * 8 + [first] * 2 + [second] * 2,
        [((D, 2 * HID), bf16)],
        out_specs=[pl.BlockSpec((D, HALF), lambda t: (0, t))],
        grid=(2 * tiles,),
        scratch=[pltpu.VMEM((D, ROW_LEN), bf16)],
        flops=4 * ROW_LEN * D * HID,
        keep=(0,),
        after=after,
    )[0]


def attn_grad_kernel(with_small, x0, x1, x2, x3, d0, d1, d2, d3, m0, m1, o0, o1, *refs):
    g_ref, t_ref = refs[-2:]
    step = pl.program_id(0)

    @pl.when(step == 0)
    def _():
        turn_into(t_ref, (x0, x1, x2, x3))

    @pl.when(step == 3)
    def _():
        turn_into(t_ref, (d0, d1, d2, d3))

    @pl.when(step < 3)
    def _():
        g_ref[...] = grad_tile(t_ref, (m0, m1))

    @pl.when(step == 3)
    def _():
        g_ref[...] = grad_tile(t_ref, (o0, o1))

    if with_small:

        @pl.when(step == 4)
        def _():
            g_ref[...] = refs[0][...]


def attn_grads(streams, dblocks, dmixes, outs, after, small=None):
    blk = whole((BLK, D))
    first = pl.BlockSpec((HALF, WIDE), lambda t: (0, jnp.minimum(t, 2)))
    args = (*streams, *dblocks, *dmixes, *outs) + (() if small is None else (small,))
    specs = [blk] * 8 + [first] * 2 + [whole((HALF, WIDE))] * 2
    specs += [] if small is None else [whole((D, WIDE))]
    steps = 4 if small is None else 5
    return call(
        functools.partial(attn_grad_kernel, small is not None),
        args,
        specs,
        [((D, steps * WIDE), bf16)],
        out_specs=[pl.BlockSpec((D, WIDE), lambda t: (0, t))],
        grid=(steps,),
        scratch=[pltpu.VMEM((D, ROW_LEN), bf16)],
        flops=2 * ROW_LEN * D * 4 * WIDE,
        after=after,
    )[0]


def loss_kernel(ls_ref, e_ref, seg_ref, segr_ref, len_ref, par_ref, x0_ref, x1_ref, we_ref,
                dx0_ref, dx1_ref, ge_ref, out_ref, sim_ref, b_ref, ll_ref, de_ref):
    tokens = ROW_LEN
    mine = HALF
    width_blk = BLK
    emb = e_ref[...].astype(f32)
    emb_t = emb.T
    lanes = lax.broadcasted_iota(jnp.int32, (tokens, PAIR), 1)
    label_col = lanes.astype(f32)
    member = (seg_ref[...] == label_col).astype(bf16)
    rows16 = lax.broadcasted_iota(jnp.int32, (16, tokens), 0).astype(f32)
    member_t = (jnp.broadcast_to(segr_ref[0:1, :], (16, tokens)) == rows16).astype(bf16)
    scale = jnp.exp(ls_ref[0])
    cls = lax.broadcasted_iota(jnp.int32, (16, PAIR), 0)
    seg = lax.broadcasted_iota(jnp.int32, (16, PAIR), 1)
    real = (cls < SEGS) & (seg < SEGS)
    allowed = (cls != seg) & real
    lengths = len_ref[0:1, :]
    chosen = (cls.astype(f32) == par_ref[0:1, :]) & real
    loss = jnp.zeros((1, PAIR), f32)
    dscale = jnp.zeros((1, PAIR), f32)
    de_ref[...] = jnp.zeros(de_ref.shape, f32)
    for width in (EMB, EMB * 3 // 4, EMB // 2):
        kept = jnp.where(lanes < width, emb, 0.0)
        r_col = lax.rsqrt(jnp.sum(kept * kept, axis=1, keepdims=True) + 1e-06)
        kept_low = kept.astype(bf16)
        row_of = lax.broadcasted_iota(jnp.int32, (PAIR, tokens), 0)
        kept_t = jnp.where(row_of < width, emb_t, 0.0)
        r_row = lax.rsqrt(jnp.sum(kept_t * kept_t, axis=0, keepdims=True) + 1e-06)
        b_ref[16:24, :] = jnp.broadcast_to(r_row, (8, tokens))

        def sims(i, carry):
            at = pl.multiple_of(i * width_blk, width_blk)
            cols = pl.ds(at, width_blk)
            other = jnp.where(lanes[0:width_blk, :] < width, e_ref[cols, :], jnp.zeros((width_blk, PAIR), bf16))
            near = dot_nt(kept_low, other)
            expo = jnp.exp(near * r_col * (b_ref[16:17, cols] * (1.0 / sharpness)) - 1.0 / sharpness)
            sim_ref[:, cols] = expo
            ll_ref[:, cols] = dot_nn(member_t, expo.astype(bf16))
            return carry

        lax.fori_loop(0, tokens // width_blk, sims, 0)
        totals = ll_ref[...]
        sum_rows = lax.broadcasted_iota(jnp.int32, totals.shape, 0)
        totals = jnp.where(sum_rows < SEGS, totals, 1.0)
        soft = sharpness * jnp.log(totals) + 1.0
        score = jnp.dot(soft, member.astype(f32), precision=best, preferred_element_type=f32) / lengths
        logits = jnp.where(allowed, scale * score, -1e30)
        top = jnp.max(logits, axis=0, keepdims=True)
        powers = jnp.exp(logits - top)
        summed = jnp.sum(powers, axis=0, keepdims=True)
        picked = jnp.sum(jnp.where(chosen, logits, 0.0), axis=0, keepdims=True)
        live = seg[0:1, :] < SEGS
        loss = loss + jnp.where(live, top + jnp.log(summed) - picked, 0.0)
        dlogit = jnp.where(allowed, powers / summed - chosen.astype(f32), 0.0)
        dscale = dscale + jnp.sum(dlogit * jnp.where(allowed, logits, 0.0), axis=0, keepdims=True)
        dscore = dlogit * scale / lengths
        dsoft = jnp.dot(dscore, jnp.concatenate([member_t.astype(f32), jnp.zeros((PAIR - 16, tokens), f32)], axis=0),
                        precision=best, preferred_element_type=f32)
        coef = dsoft / totals
        b_ref[0:16, :] = coef
        coef_high, coef_rest = halves(coef)
        left = jnp.concatenate([member_t, member_t, coef_high, coef_rest], axis=0)
        keep_t = kept_t.astype(bf16)

        def pulls(i, carry):
            at = pl.multiple_of(i * width_blk, width_blk)
            cols = pl.ds(at, width_blk)
            here_high, here_rest = halves(b_ref[0:16, cols])
            member_here = (
                jnp.broadcast_to(segr_ref[0:1, cols], (16, width_blk)) == rows16[:, 0:width_blk]
            ).astype(bf16)
            right = jnp.concatenate([here_high, here_rest, member_here, member_here], axis=0)
            pull = dot_tn(left, right) * sim_ref[:, cols] * r_col
            high, rest = halves(pull)
            de = dot_nn(keep_t, high) + dot_nn(keep_t, rest)
            r_here = b_ref[16:17, cols]
            e_here = jnp.where(lanes[0:width_blk, :] < width, e_ref[cols, :].astype(f32), 0.0).T
            along = jnp.sum(e_here * de, axis=0, keepdims=True)
            de_ref[:, cols] += r_here * de - (r_here * r_here * r_here * along) * e_here
            return carry

        lax.fori_loop(0, mine // width_blk, pulls, 0)
    de = de_ref[...].T.astype(bf16)
    dx0_ref[...] = dot_nt(de[0:BLK, :], we_ref[...])
    dx1_ref[...] = dot_nt(de[BLK:HALF, :], we_ref[...])
    ge_ref[...] = dot_tn(x0_ref[...], de[0:BLK, :]) + dot_tn(x1_ref[...], de[BLK:HALF, :])
    out_ref[...] = jnp.concatenate([loss, dscale, jnp.zeros((6, PAIR), f32)], axis=0)


def loss_and_grads(log_scale, emb, seg_col, seg_row, lengths, partner, x0, x1, w_emb):
    blk = whole((BLK, D))
    return call(
        loss_kernel,
        (log_scale, emb, seg_col, seg_row, lengths, partner, x0, x1, w_emb),
        [
            smem(), whole((ROW_LEN, EMB)), whole((ROW_LEN, PAIR)), whole((8, ROW_LEN)),
            whole((8, PAIR)), whole((8, PAIR)), blk, blk, whole((D, EMB)),
        ],
        [((BLK, D), f32), ((BLK, D), f32), ((D, EMB), f32), ((8, PAIR), f32)],
        scratch=[
            pltpu.VMEM((ROW_LEN, ROW_LEN), f32),
            pltpu.VMEM((24, ROW_LEN), f32),
            pltpu.VMEM((16, ROW_LEN), f32),
            pltpu.VMEM((EMB, HALF), f32),
        ],
        flops=20 * ROW_LEN * ROW_LEN * EMB,
    )


def row_layout(lengths):
    ends = jnp.cumsum(lengths)
    places = jnp.arange(ROW_LEN, dtype=jnp.int32)
    after = places[:, None] >= ends[None, :]
    segment = jnp.sum(after.astype(jnp.int32), axis=1)
    starts = jnp.sum(jnp.where(after, lengths[None, :], 0), axis=1)
    return (segment, places - starts)


def adamw_update(master, moments, grad, factor, rate, step_f):
    scaled = grad * factor
    moment_one = 0.9 * moments[0] + 0.1 * scaled
    moment_two = 0.95 * moments[1] + 0.05 * scaled * scaled
    one_hat = moment_one / (1.0 - jnp.power(0.9, step_f))
    two_hat = moment_two / (1.0 - jnp.power(0.95, step_f))
    updated = master - rate * (one_hat / (jnp.sqrt(two_hat) + 1e-08) + 0.01 * master)
    return (updated, moment_one, moment_two)


def adam_kernel(rate, turned, k_ref, w_ref, m_ref, v_ref, g0_ref, g1_ref, wo_ref, mo_ref, vo_ref):
    grad = jnp.where(pl.program_id(0) == 0, g0_ref[...].astype(f32), g1_ref[...].astype(f32))
    if turned:
        grad = grad.T
    scale_grad = k_ref[0:1, 1:2]
    norm = jnp.sqrt(k_ref[0:1, 0:1] + scale_grad * scale_grad + 1e-06)
    grad = (grad * (clip_limit / jnp.maximum(norm, clip_limit))).reshape(w_ref.shape)
    one = 0.9 * m_ref[...].reshape(w_ref.shape) + 0.1 * grad
    two = 0.95 * v_ref[...].reshape(w_ref.shape) + 0.05 * grad * grad
    w = w_ref[...]
    one_hat = one * (1.0 / (1.0 - 0.9 ** STEP))
    two_hat = two * (1.0 / (1.0 - 0.95 ** STEP))
    wo_ref[...] = w - rate * (one_hat / (jnp.sqrt(two_hat) + 1e-08) + 0.01 * w)
    mo_ref[...] = one
    vo_ref[...] = two


def adam_step(factor, master, moments, grads, tiles, block, where_of, grad_block, grad_at, rate, turned=False):
    spec = pl.BlockSpec((1,) + block, lambda l, t: (l,) + where_of(t))
    first = pl.BlockSpec((1, 1) + block, lambda l, t: (0, l) + where_of(t))
    second = pl.BlockSpec((1, 1) + block, lambda l, t: (1, l) + where_of(t))
    at_zero, at_one = grad_at
    return call(
        functools.partial(adam_kernel, rate, turned),
        (factor, master, moments, moments, *grads),
        [
            whole((8, PAIR)), spec, first, second,
            pl.BlockSpec(grad_block, lambda l, t: (0, at_zero + t)),
            pl.BlockSpec(grad_block, lambda l, t: (0, at_one + t)),
        ],
        [(master.shape, f32)] * 3,
        out_specs=[spec] * 3,
        grid=(LAYERS, tiles),
        flops=20 * master.size,
    )


def swap(values, axis, bit):
    count = lax.axis_size(axis)
    return lax.ppermute(values, axis, [(i, i ^ bit) for i in range(count)])


def bit_orders(axis):
    count = lax.axis_size(axis).bit_length() - 1
    return list(range(count)), list(range(1, count)) + [0]


def swap_core(values, pieces=2):
    parts = jnp.split(values, pieces, axis=0)
    return jnp.concatenate([swap(part, "mp", 1) for part in parts], axis=0)


def gather_rows(values, axis, order):
    index = lax.axis_index(axis)
    share = values.shape
    for bit in order:
        other = swap(values, axis, 1 << bit)
        high = ((index >> bit) & 1) == 1
        values = jnp.stack([jnp.where(high, other, values), jnp.where(high, values, other)])
    done = list(reversed(order))
    count = len(order)
    turn = [done.index(bit) for bit in reversed(range(count))]
    values = values.transpose(turn + [count, count + 1])
    return values.reshape((-1,) + share[1:])


def gather_both(values, axis):
    first, second = bit_orders(axis)
    cut = (values.shape[1] // 2 + PAIR - 1) // PAIR * PAIR
    parts = [
        gather_rows(values[:, :cut], axis, first[::-1]),
        gather_rows(values[:, cut:], axis, second[::-1]),
    ]
    return jnp.concatenate(parts, axis=1)


class Scatter:

    def __init__(self, values, axis, cut=None):
        orders = bit_orders(axis)
        count = len(orders[0])
        self.axis, self.index, self.steps = axis, lax.axis_index(axis), count
        cut = values.shape[1] // 2 if cut is None else cut
        parts = (values[:, :cut], values[:, cut:])
        self.parts = [p.reshape((2,) * count + (-1, p.shape[1])) for p in parts]
        self.left = [list(order) for order in orders]

    def send(self):
        self.kept, self.came = [], []
        for values, left in zip(self.parts, self.left):
            bit = left[0]
            high = ((self.index >> bit) & 1) == 1
            at = sum(1 for other in left if other > bit)
            low_part = lax.index_in_dim(values, 0, at, keepdims=False)
            high_part = lax.index_in_dim(values, 1, at, keepdims=False)
            self.kept.append(jnp.where(high, high_part, low_part))
            self.came.append(swap(jnp.where(high, low_part, high_part), self.axis, 1 << bit))

    def wait_with(self, other):
        first, second, other = lax.optimization_barrier((self.came[0], self.came[1], other))
        self.came = [first, second]
        return other

    def add(self):
        self.left = [left[1:] for left in self.left]
        parts = [k.astype(f32) + c.astype(f32) for k, c in zip(self.kept, self.came)]
        self.parts = parts if not self.left[0] else [p.astype(bf16) for p in parts]

    def result(self):
        return jnp.concatenate(self.parts, axis=1)


def sum_all(values):
    for axis in ("mp", "dp"):
        bit = 1
        while bit < lax.axis_size(axis):
            if 2 * bit < lax.axis_size(axis):
                first, second, both = [swap(values, axis, at) for at in (bit, 2 * bit, 3 * bit)]
                values = (values + first) + (second + both)
                bit *= 4
            else:
                values = values + swap(values, axis, bit)
                bit *= 2
    return values


def body(
    hidden_in,
    seg_lengths,
    partner,
    qkv_weight,
    out_weight,
    up_weight,
    down_weight,
    norm_params,
    emb_weight,
    log_scale,
    qkv_moments,
    out_moments,
    up_moments,
    down_moments,
    norm_moments,
    emb_moments,
    scale_moments,
):
    share = qkv_weight.shape[1]
    mp_count = lax.axis_size("mp")
    place = lax.axis_index("mp")
    core = place & 1
    far_chip = (place >> 1) == 1
    core_arr = core.reshape(1).astype(jnp.int32)

    def mine(first, second):
        return jnp.where(far_chip, second, first)

    def attn_pack(layer_at):
        return [qkv_weight[layer_at].reshape(share, 3 * WIDE), out_weight[layer_at].T]

    def mlp_pack(layer_at):
        return [up_weight[layer_at], down_weight[layer_at].T]

    norm_cols = jnp.pad(norm_params.reshape(4 * LAYERS, share).T, ((0, 0), (0, PAIR - 4 * LAYERS)))

    def packed(parts):
        return jnp.concatenate(parts, axis=1).astype(bf16)

    def gather(values):
        return lax.all_gather(values, "dp", axis=0, tiled=True)

    first_w = gather_both(packed(attn_pack(0) + [norm_cols]), "dp")
    middle_w = gather(packed(attn_pack(1) + mlp_pack(0)))
    last_w = gather(packed(mlp_pack(1) + [emb_weight]))
    attn_w = [first_w, middle_w]
    mlp_w = [(middle_w, 1), (last_w, 0)]
    nrm = first_w[:, 4 * WIDE : 4 * WIDE + 4 * LAYERS].T.astype(f32)
    w_emb = last_w[:, 2 * HID :]

    segment, offset = row_layout(seg_lengths[0])

    def own_order(values):
        blocks = values.reshape(2, 2, BLK)
        return jnp.where(core == 1, blocks[:, ::-1], blocks).reshape(ROW_LEN)

    segment = own_order(segment).astype(f32)
    offset = own_order(offset).astype(f32)
    seg_col = jnp.broadcast_to(segment[:, None], (ROW_LEN, PAIR))
    seg_row = jnp.broadcast_to(segment[None, :], (8, ROW_LEN))
    lane = jnp.arange(PAIR, dtype=jnp.int32)
    frequency = jnp.exp((lane % (HEAD_DIM // 2)).astype(f32) * (-2.0 * math.log(10000.0) / HEAD_DIM))
    angles = offset[:, None] * frequency[None, :]
    cosines = jnp.cos(angles)
    sines = jnp.where((lane % HEAD_DIM) < HEAD_DIM // 2, -1.0, 1.0)[None, :] * jnp.sin(angles)

    other_half = swap(hidden_in, "mp", 2)
    low = [mine(hidden_in, other_half), mine(other_half, hidden_in)]
    stream = [v.astype(f32) for v in low]

    def chip_sum(own, send):
        return (own.astype(f32) + swap_core(send).astype(f32)).astype(bf16)

    def cross(total, earlier=None):
        if earlier is not None:
            total, earlier = lax.optimization_barrier((total, earlier))
        return total, swap(total, "mp", 2), earlier

    kept = []
    sums = None
    for layer_at in range(LAYERS):
        streams, qkvs, norm_prev = [], [], []
        if layer_at > 0:
            stream, low = [], []
        for at in range(2):
            if layer_at > 0:
                h, hb, zz = norm_fwd(4 * layer_at - 2, normed[at], *sums[at], nrm)
                stream.append(h)
                low.append(hb)
                kept[-1][-1].append(zz)
            sib = swap_core(low[at])
            streams += [low[at], sib]
            qkvs.append(qkv_project(low[at], sib, attn_w[layer_at], cosines, sines, at))
        o_a, lse_a, own, send = attend(
            0, core_arr, qkvs[0], qkvs[1], seg_col, seg_row, attn_w[layer_at], None
        )
        total_a, came_a, _ = cross(chip_sum(own, send))
        o_b, lse_b, own, send = attend(
            1, core_arr, qkvs[1], qkvs[0], seg_col, seg_row, attn_w[layer_at], total_a
        )
        total_b, came_b, came_a = cross(chip_sum(own, send), came_a)
        h_a, hb_a, z_a = norm_fwd(4 * layer_at, stream[0], total_a, came_a, nrm)
        sib_a = swap_core(hb_a)
        zg_a, own, send = mlp(hb_a, sib_a, mlp_w[layer_at], None)
        next_a, next_came_a, came_b = cross(chip_sum(own, send), came_b)
        h_b, hb_b, z_b = norm_fwd(4 * layer_at, stream[1], total_b, came_b, nrm)
        sib_b = swap_core(hb_b)
        zg_b, own, send = mlp(hb_b, sib_b, mlp_w[layer_at], None)
        next_b, next_came_b, next_came_a = cross(chip_sum(own, send), next_came_a)
        normed = [h_a, h_b]
        sums = [(next_a, next_came_a), (next_b, next_came_b)]
        kept.append(
            (streams, qkvs, [(o_a, lse_a), (o_b, lse_b)], [z_a, z_b], [hb_a, sib_a, hb_b, sib_b], [zg_a, zg_b], [])
        )
    stream, low = [], []
    for at in range(2):
        h, hb, zz = norm_fwd(4 * LAYERS - 2, normed[at], *sums[at], nrm)
        stream.append(h)
        low.append(hb)
        kept[-1][-1].append(zz)
    hidden_out = mine(stream[0], stream[1])

    emb_own = jnp.concatenate([dot_nn(low[0], w_emb), dot_nn(low[1], w_emb)], axis=0).astype(bf16)
    emb_all = jnp.concatenate([emb_own, swap(emb_own, "mp", 1)], axis=0)

    def loss_order(values):
        return values.reshape(2, 2, BLK).transpose(1, 0, 2).reshape(ROW_LEN)

    loss_seg = loss_order(segment)
    lengths = jnp.broadcast_to(
        jnp.pad(seg_lengths[0].astype(f32), (0, PAIR - SEGS), constant_values=1.0)[None], (8, PAIR)
    )
    partners = jnp.broadcast_to(
        jnp.pad(partner[0].astype(f32), (0, PAIR - SEGS), constant_values=-1.0)[None], (8, PAIR)
    )
    dx0, dx1, g_emb, loss_parts = loss_and_grads(
        log_scale,
        emb_all,
        jnp.broadcast_to(loss_seg[:, None], (ROW_LEN, PAIR)),
        jnp.broadcast_to(loss_seg[None, :], (8, ROW_LEN)),
        lengths,
        partners,
        low[0],
        low[1],
        w_emb,
    )

    grads = [dx0, dx1]
    pending = [(), ()]
    reduced = []
    norm_grads = [None] * LAYERS
    for layer_at in reversed(range(LAYERS)):
        streams, qkvs, attended, norm_a, hiddens, zgs, norm_b = kept[layer_at]
        row = 4 * layer_at + 2
        d_a, db_a, gain_a = norm_bwd(row, grads[0], pending[0], norm_b[0], nrm)
        sib_a = swap_core(db_a)
        du_a, own, send = mlp_back(db_a, sib_a, zgs[0], mlp_w[layer_at], None)
        total_a = chip_sum(own, send)
        if pending[1]:
            total_a, came_a, came_b = cross(total_a, pending[1][1])
            if upper.left[0]:
                came_b = upper.wait_with(came_b)
                upper.add()
                upper.send()
            pending[1] = (pending[1][0], came_b)
        else:
            total_a, came_a, _ = cross(total_a)
        d_b, db_b, gain_b = norm_bwd(row, grads[1], pending[1], norm_b[1], nrm)
        sib_b = swap_core(db_b)
        du_b, own, send = mlp_back(db_b, sib_b, zgs[1], mlp_w[layer_at], total_a)
        total_b, came_b, came_a = cross(chip_sum(own, send), came_a)
        gains = [(gain_a + gain_b)[:2]]
        both = mlp_grads(hiddens, [db_a, sib_a, db_b, sib_b], [du_a, du_b], zgs, total_b)
        both, came_b = lax.optimization_barrier((both, came_b))
        reduced.append(lax.psum_scatter(both, "dp", scatter_dimension=0, tiled=True))
        row = 4 * layer_at
        grad_a, low_a, gain_a = norm_bwd(row, d_a, (total_a, came_a), norm_a[0], nrm)
        sib_a = swap_core(low_a)
        if layer_at < LAYERS - 1:
            came_b = upper.wait_with(came_b)
            upper.add()
            upper.send()
        grad_b, low_b, gain_b = norm_bwd(row, d_b, (total_b, came_b), norm_a[1], nrm)
        dattn = [low_a, sib_a, low_b, swap_core(low_b)]
        dmixes = attend_back(
            core_arr, dattn, attn_w[layer_at], *qkvs, attended[0][0], attended[1][0],
            attended[0][1], attended[1][1], seg_col, seg_row, cosines, sines,
        )
        norm_grads[layer_at] = jnp.concatenate([(gain_a + gain_b)[:2]] + gains, axis=0)
        outs = [attended[0][0], attended[1][0]]
        grads = [grad_a, grad_b]
        if layer_at > 0:
            total_a, came_a, _ = cross(chip_sum(*qkv_back(dmixes[0], attn_w[layer_at], None)))
            above = attn_grads(streams, dattn, dmixes, outs, total_a)
            above, came_a = lax.optimization_barrier((above, came_a))
            upper = Scatter(above, "dp")
            upper.send()
            total_b, came_b, came_a = cross(
                chip_sum(*qkv_back(dmixes[1], attn_w[layer_at], total_a)), came_a
            )
            pending = [(total_a, came_a), (total_b, came_b)]
        else:
            norm_rows = jnp.concatenate(norm_grads, axis=0)
            small = jnp.concatenate([g_emb, jnp.pad(norm_rows.T, ((0, 0), (0, PAIR - 4 * LAYERS)))], axis=1)
            last = attn_grads(streams, dattn, dmixes, outs, None, small.astype(bf16))
            lower = Scatter(last, "dp")
            squares = jnp.sum(jnp.square(reduced[0].astype(f32)))
            while lower.left[0]:
                lower.send()
                if len(lower.left[0]) == lower.steps:
                    squares = upper.wait_with(lower.wait_with(squares))
                    while upper.left[0]:
                        upper.add()
                        if upper.left[0]:
                            upper.send()
                    fourth = upper.result()
                    squares = squares + jnp.sum(jnp.square(fourth))
                lower.add()
            third = lower.result()
            totals = []
            for at in range(2):
                own, send = qkv_back(dmixes[at], attn_w[layer_at], last)
                totals.append(own.astype(f32) + swap(send, "mp", 1).astype(f32))
            came = swap(mine(totals[1], totals[0]).astype(bf16), "mp", 2)
            hidden_grad = mine(grads[0], grads[1]) + (mine(totals[0], totals[1]) + came.astype(f32))

    first, second = reduced
    third, hidden_grad = lax.optimization_barrier((third, hidden_grad))
    small = third[:, 4 * WIDE :]
    small = small + swap(small, "mp", 1)
    emb_grad = small[:, :EMB]
    norm_grad = small[:, EMB : EMB + 4 * LAYERS].T.reshape(LAYERS, 2, 2, share)
    squares = (
        squares + jnp.sum(jnp.square(second.astype(f32))) + jnp.sum(jnp.square(third[:, : 4 * WIDE]))
        + jnp.sum(small * small) / mp_count
    )
    parts = jnp.concatenate([loss_parts[:2], jnp.zeros((6, PAIR), f32)], axis=0)
    loss_here = jnp.sum(parts[0]) / mp_count
    dscale_here = jnp.sum(parts[1]) / mp_count
    vector = jnp.where(lane == 0, squares, jnp.where(lane == 1, dscale_here, jnp.where(lane == 2, loss_here, 0.0)))
    vector = sum_all(jnp.broadcast_to(vector[None], (8, PAIR)))
    total_squares = vector[0, 0]
    scale_grad = vector[0, 1:2]
    loss_total = vector[0, 2]
    norm_value = jnp.sqrt(total_squares + scale_grad[0] * scale_grad[0] + 1e-06)
    factor = clip_limit / jnp.maximum(norm_value, clip_limit)
    step_f = jnp.asarray(STEP, f32)
    qkv_step = adam_step(
        vector, qkv_weight.transpose(0, 2, 1, 3), qkv_moments.transpose(0, 1, 3, 2, 4), (third, fourth),
        3, (1, share, WIDE), lambda t: (t, 0, 0), (share, WIDE), (0, 0), D ** (-0.5),
    )
    qkv_new, qkv_first, qkv_second = [v.transpose(0, 2, 1, 3) for v in qkv_step]
    out_new, out_first, out_second = adam_step(
        vector, out_weight, out_moments, (third, fourth),
        1, (WIDE, share), lambda t: (t, 0), (share, WIDE), (3, 3), (D * SEGS // ROW_LEN) ** (-0.5), True,
    )
    up_new, up_first, up_second = adam_step(
        vector, up_weight, up_moments, (second, first),
        2, (share, HALF), lambda t: (0, t), (share, HALF), (0, 0), D ** (-0.5),
    )
    down_new, down_first, down_second = adam_step(
        vector, down_weight, down_moments, (second, first),
        4, (TILE, share), lambda t: (t, 0), (share, TILE), (4, 4), FF ** (-0.5), True,
    )
    norm_new, norm_first, norm_second = adamw_update(norm_params, norm_moments, norm_grad, factor, 0.5, step_f)
    emb_new, emb_first, emb_second = adamw_update(emb_weight, emb_moments, emb_grad, factor, D ** (-0.5), step_f)
    scale_new, scale_first, scale_second = adamw_update(log_scale, scale_moments, scale_grad, factor, 1.0, step_f)
    return (
        hidden_out,
        hidden_grad,
        loss_total.reshape(1),
        norm_value.reshape(1),
        qkv_new,
        qkv_first,
        qkv_second,
        out_new,
        out_first,
        out_second,
        up_new,
        up_first,
        up_second,
        down_new,
        down_first,
        down_second,
        norm_new,
        norm_first,
        norm_second,
        emb_new,
        emb_first,
        emb_second,
        scale_new,
        scale_first,
        scale_second,
    )


def solution(mesh):
    placed = (
        P(("dp", "mp"), None),
        P("dp", None),
        P("dp", None),
        P(None, "dp", None, "mp"),
        P(None, "mp", "dp"),
        P(None, "dp", "mp"),
        P(None, "mp", "dp"),
        P(None, None, None, "dp"),
        P("dp", None),
        P(),
        P(None, None, "dp", None, "mp"),
        P(None, None, "mp", "dp"),
        P(None, None, "dp", "mp"),
        P(None, None, "mp", "dp"),
        P(None, None, None, None, "dp"),
        P(None, "dp", None),
        P(),
    )
    results = (P(("dp", "mp"), None), P(("dp", "mp"), None), P(), P())
    for at in (3, 4, 5, 6, 7, 8, 9):
        results += (placed[at],) * 3
    return jax.shard_map(body, mesh=mesh, in_specs=placed, out_specs=results, check_vma=False)
```
